32 devices in a mesh: gx: 4 (over y, x), gy: 2 (over core), ha: 4 (over z).
Axes of the slice: x: 2, y: 2, z: 4, core: 2. Of those that a mesh axis runs over, the one named last changes fastest.
Arguments:
- level_set: float32 [32, 32, 40, 128], P('gx', 'gy', 'ha'), may hold values from -4 to 4
- wind_field: float32 [2, 32, 32], P(None, 'gx', 'gy'), may hold values from -3 to 3
Outputs:
- increment: float32 [32, 32, 40, 128], P('gx', 'gy', 'ha')
The draws below stay inside these ranges and needn't reach their ends.
All inputs are finite; a program needn't handle non-finite values.
Results may differ from the reference program's by a relative error of at most 0.000073.
Values sent between devices are 32-bit elements; how exact they have to be, the bound alone decides.
No kernel may reach another device: no remote copies, remote signals or barrier semaphores. Data moves between devices by JAX's collectives and lax.ppermute only.
A program may use at most 128 MiB of HBM per device.

```python
import math
import jax
import jax.numpy as jnp
from jax import lax

NV = 128
NX = 32
NY = 32
NH = 40


CELL_SIZE = 0.05


def draw_level_set(key, part):
    rough_key = jax.random.fold_in(key, 11)
    center_key = jax.random.fold_in(key, 12)
    shape = (NX, NY, NH, NV)
    centers = jax.random.uniform(center_key, (2,), jnp.float32, 0.3, 0.7)
    pos_x = (jnp.arange(NX, dtype=jnp.float32) + 0.5) / NX
    pos_y = (jnp.arange(NY, dtype=jnp.float32) + 0.5) / NY
    span_x = (pos_x - centers[0]) * NX * CELL_SIZE
    span_y = (pos_y - centers[1]) * NY * CELL_SIZE
    smooth = jnp.sqrt(span_x[:, None] ** 2 + span_y[None, :] ** 2 + 0.01) - 0.25 * NX * CELL_SIZE
    smooth = smooth[:, :, None, None]
    rough = 0.5 * jax.random.normal(rough_key, shape, jnp.float32)
    surface = rough + smooth
    return jnp.clip(surface, -4.0, 4.0)


def draw_wind_field(key, part):
    raw_key = jax.random.fold_in(key, 21)
    shape = (2, NX, NY)
    ramp = 0.1 + 2.9 * (jnp.arange(NX, dtype=jnp.float32) + 0.5) / NX
    raw = jax.random.uniform(raw_key, shape, jnp.float32, -1.0, 1.0)
    return raw * ramp[None, :, None]


def setup_inputs(seed: int = 0) -> dict:
    streams_of = jax.random.split(jax.random.key(seed), 3)
    return {
        "level_set": draw_level_set(jax.random.fold_in(streams_of[2], 71), 0),
        "wind_field": draw_wind_field(jax.random.fold_in(streams_of[2], 71), 0),
    }


CELL_SIZE = 0.05
SPEED_LOW = 0.1
SPEED_SPAN = 0.4
TURN_MAX = 1.0
ACCEL_MAX = 0.05
CFL_NUMBER = 0.5
WENO_EPS = 1e-6


def ghost_rows(values, along, at_low):
    length = values.shape[along]
    if at_low:
        edge_row = lax.slice_in_dim(values, 0, 1, axis=along)
        next_row = lax.slice_in_dim(values, 1, 2, axis=along)
        reaches = (3.0, 2.0, 1.0)
    else:
        edge_row = lax.slice_in_dim(values, length - 1, length, axis=along)
        next_row = lax.slice_in_dim(values, length - 2, length - 1, axis=along)
        reaches = (1.0, 2.0, 3.0)
    slope_edge = edge_row - next_row
    return jnp.concatenate([edge_row + distance * slope_edge for distance in reaches], axis=along)


def extend(values, along):
    return jnp.concatenate([ghost_rows(values, along, True), values, ghost_rows(values, along, False)], axis=along)


def speed_shifts(values):
    length = values.shape[3]
    below_rows = ghost_rows(values, 3, True)
    above_rows = ghost_rows(values, 3, False)
    shifted = []
    for displace in range(-3, 4):
        pieces = []
        if displace < 0:
            pieces.append(lax.slice_in_dim(below_rows, 3 + displace, 3, axis=3))
        pieces.append(lax.slice_in_dim(values, max(displace, 0), length + min(displace, 0), axis=3))
        if displace > 0:
            pieces.append(lax.slice_in_dim(above_rows, 0, displace, axis=3))
        shifted.append(jnp.concatenate(pieces, axis=3) if len(pieces) > 1 else pieces[0])
    return shifted


def weno_side(left_far, left_near, middle, right_near, right_far):
    guess_one = left_far * (1.0 / 3.0) - left_near * (7.0 / 6.0) + middle * (11.0 / 6.0)
    guess_two = -left_near * (1.0 / 6.0) + middle * (5.0 / 6.0) + right_near * (1.0 / 3.0)
    guess_three = middle * (1.0 / 3.0) + right_near * (5.0 / 6.0) - right_far * (1.0 / 6.0)
    smooth_one = (13.0 / 12.0) * jnp.square(left_far - 2.0 * left_near + middle) + 0.25 * jnp.square(left_far - 4.0 * left_near + 3.0 * middle)
    smooth_two = (13.0 / 12.0) * jnp.square(left_near - 2.0 * middle + right_near) + 0.25 * jnp.square(left_near - right_near)
    smooth_three = (13.0 / 12.0) * jnp.square(middle - 2.0 * right_near + right_far) + 0.25 * jnp.square(3.0 * middle - 4.0 * right_near + right_far)
    weight_one = 0.1 / jnp.square(smooth_one + WENO_EPS)
    weight_two = 0.6 / jnp.square(smooth_two + WENO_EPS)
    weight_three = 0.3 / jnp.square(smooth_three + WENO_EPS)
    return (weight_one * guess_one + weight_two * guess_two + weight_three * guess_three) / (weight_one + weight_two + weight_three)


def weno_pair(shifted, spacing):
    slopes = [(shifted[position + 1] - shifted[position]) / spacing for position in range(6)]
    left_slope = weno_side(slopes[0], slopes[1], slopes[2], slopes[3], slopes[4])
    right_slope = weno_side(slopes[5], slopes[4], slopes[3], slopes[2], slopes[1])
    return left_slope, right_slope


def cell_rates(cos_head, sin_head, speeds, wind_x, wind_y, d_theta, d_speed):
    along_x = speeds[None, None, None, :] * cos_head[None, None, :, None] + wind_x[:, :, None, None]
    along_y = speeds[None, None, None, :] * sin_head[None, None, :, None] + wind_y[:, :, None, None]
    return jnp.abs(along_x) / CELL_SIZE + jnp.abs(along_y) / CELL_SIZE + TURN_MAX / d_theta + ACCEL_MAX / d_speed


def hamilton(x_pair, y_pair, head_pair, speed_pair, cos_head, sin_head, speeds, wind_x, wind_y):
    flow_x = speeds[None, None, None, :] * cos_head[None, None, :, None] + wind_x[:, :, None, None]
    flow_y = speeds[None, None, None, :] * sin_head[None, None, :, None] + wind_y[:, :, None, None]
    mean_x = 0.5 * (x_pair[0] + x_pair[1])
    mean_y = 0.5 * (y_pair[0] + y_pair[1])
    mean_head = 0.5 * (head_pair[0] + head_pair[1])
    mean_speed = 0.5 * (speed_pair[0] + speed_pair[1])
    value = -(flow_x * mean_x + flow_y * mean_y + TURN_MAX * jnp.abs(mean_head) + ACCEL_MAX * jnp.abs(mean_speed))
    damping = 0.5 * (jnp.abs(flow_x) * (x_pair[1] - x_pair[0]) + jnp.abs(flow_y) * (y_pair[1] - y_pair[0])
                     + TURN_MAX * (head_pair[1] - head_pair[0]) + ACCEL_MAX * (speed_pair[1] - speed_pair[0]))
    return -jnp.maximum(value - damping, 0.0)


def reference(level_set, wind_field):
    d_theta = 2.0 * math.pi / NH
    d_speed = SPEED_SPAN / NV
    angles = jnp.arange(NH, dtype=jnp.int32).astype(jnp.float32) * d_theta
    cos_head = jnp.cos(angles)
    sin_head = jnp.sin(angles)
    speeds = SPEED_LOW + SPEED_SPAN * (jnp.arange(NV, dtype=jnp.int32).astype(jnp.float32) + 0.5) / NV
    rows_all = jnp.arange(NX, dtype=jnp.int32)

    def plane_max(position):
        winds = lax.dynamic_slice_in_dim(wind_field, position, 1, 1)
        return jnp.max(cell_rates(cos_head, sin_head, speeds, winds[0], winds[1], d_theta, d_speed))

    time_step = CFL_NUMBER / jnp.max(lax.map(plane_max, rows_all))

    def advance(surface):
        x_padded = extend(surface, 0)

        def one_plane(position):
            x_plane = lax.dynamic_slice_in_dim(surface, position, 1, 0)
            x_shifted = [lax.dynamic_slice_in_dim(x_padded, position + 3 + displace, 1, 0) for displace in range(-3, 4)]
            y_padded = extend(x_plane, 1)
            y_shifted = [y_padded[:, 3 + displace:3 + displace + NY] for displace in range(-3, 4)]
            head_padded = jnp.concatenate([x_plane[:, :, NH - 3:], x_plane, x_plane[:, :, :3]], axis=2)
            head_shifted = [head_padded[:, :, 3 + displace:3 + displace + NH] for displace in range(-3, 4)]
            winds = lax.dynamic_slice_in_dim(wind_field, position, 1, 1)
            return hamilton(weno_pair(x_shifted, CELL_SIZE), weno_pair(y_shifted, CELL_SIZE),
                            weno_pair(head_shifted, d_theta), weno_pair(speed_shifts(x_plane), d_speed),
                            cos_head, sin_head, speeds, winds[0], winds[1])

        return lax.map(one_plane, rows_all).reshape(surface.shape)

    section_one = level_set + time_step * advance(level_set)
    section_two = 0.75 * level_set + 0.25 * (section_one + time_step * advance(section_one))
    advanced = (1.0 / 3.0) * level_set + (2.0 / 3.0) * (section_two + time_step * advance(section_two))
    return advanced - level_set
```

```python
import functools
import math

import jax
import jax.numpy as jnp
import numpy as np
from jax import lax
from jax.experimental import pallas as pl
from jax.experimental.pallas import tpu as pltpu
from jax.sharding import PartitionSpec as P

CELL_SIZE = 0.05
SPEED_LOW = 0.1
SPEED_SPAN = 0.4
TURN_MAX = 1.0
ACCEL_MAX = 0.05
CFL_NUMBER = 0.5
WENO_EPS = 1e-06
SUB = 8
LANES = 128


def weno_terms(us, eps):
    n = len(us) - 6
    u = {i - 3: v for i, v in enumerate(us)}
    q = {r: u[r] - u[r - 1] for r in range(-2, n + 3)}
    p = {m: q[m + 1] - q[m] for m in range(-2, n + 2)}
    t, alpha, beta, gamma, a3, g3 = {}, {}, {}, {}, {}, {}
    for r in range(-1, n + 2):
        t[r] = p[r] - p[r - 1]
        z = 1.5 * t[r]
        base = t[r] * t[r] + ((0.75 * p[r - 1]) * p[r] + eps)
        if r <= n - 1:
            s = base + p[r] * z
            alpha[r] = pl.reciprocal(s * s, approx=APPROX)
            a3[r] = (1.0 / 3.0) * alpha[r]
        if r >= 1:
            s = base - p[r - 1] * z
            gamma[r] = pl.reciprocal(s * s, approx=APPROX)
            g3[r] = (1.0 / 3.0) * gamma[r]
        if 0 <= r <= n:
            beta[r] = pl.reciprocal(0.5 * (base * base), approx=APPROX)
    f = {m: t[m] - t[m + 1] for m in range(-1, n + 1)}
    f2 = {m: f[m] + f[m] for m in range(-1, n + 1)}
    return n, q, p, alpha, beta, gamma, a3, g3, f, f2


APPROX = True


def line_max(us, eps, scale):
    n, q, p, alpha, beta, gamma, a3, g3, f, f2 = weno_terms(us, eps)
    outs = []
    for i in range(n):
        er = (g3[i + 2] * f2[i + 1] + alpha[i] * f[i]) * pl.reciprocal(
            g3[i + 2] + beta[i + 1] + alpha[i], approx=APPROX
        )
        el = (a3[i - 1] * f2[i - 1] + gamma[i + 1] * f[i]) * pl.reciprocal(
            a3[i - 1] + beta[i] + gamma[i + 1], approx=APPROX
        )
        p2 = p[i] + p[i]
        right = (6.0 * q[i + 1] - p2) - (p[i + 1] + er)
        minus_left = -(6.0 * q[i] + p2) - (p[i - 1] + el)
        outs.append(scale * jnp.maximum(right, minus_left))
    return outs


def line_upwind(us, eps, flows):
    n, q, p, alpha, beta, gamma, a3, g3, f, f2 = weno_terms(us, eps)
    outs = []
    for i in range(n):
        flow = flows(i)
        right = flow > 0.0
        w1 = jnp.where(right, g3[i + 2], a3[i - 1])
        w2 = jnp.where(right, beta[i + 1], beta[i])
        w3 = jnp.where(right, alpha[i], gamma[i + 1])
        f1 = jnp.where(right, f2[i + 1], f2[i - 1])
        pn = jnp.where(right, p[i + 1], p[i - 1])
        qn = jnp.where(right, q[i + 1], q[i])
        e = (w1 * f1 + w3 * f[i]) * pl.reciprocal(w1 + w2 + w3, approx=APPROX)
        x = pn + (p[i] + p[i]) + e
        outs.append(flow * qn - jnp.abs((1.0 / 6.0) * flow) * x)
    return outs


def edge_fix(low, center_low, center_high, high, flags):
    first, last = flags
    slope = center_low[0] - center_low[1]
    low = [
        jnp.where(first, center_low[0] + reach * slope, got)
        for reach, got in zip((3.0, 2.0, 1.0), low)
    ]
    slope = center_high[1] - center_high[0]
    high = [
        jnp.where(last, center_high[1] + reach * slope, got)
        for reach, got in zip((1.0, 2.0, 3.0), high)
    ]
    return low, high


def speed_kernel(u_ref, acc_ref, line_ref, out_ref, *, eps, scale):
    rows = u_ref.shape[0]
    count = LANES // SUB

    def group(g, carry):
        base = pl.multiple_of(g * LANES, LANES)
        turned = u_ref[pl.ds(base, LANES), :].T
        line_ref[pl.ds(SUB, LANES), :] = turned
        slope = turned[0:1] - turned[1:2]
        for reach in (1, 2, 3):
            line_ref[pl.ds(SUB - reach, 1), :] = turned[0:1] + float(reach) * slope
        slope = turned[LANES - 1 :] - turned[LANES - 2 : LANES - 1]
        for reach in (1, 2, 3):
            line_ref[pl.ds(SUB + LANES - 1 + reach, 1), :] = turned[LANES - 1 :] + float(reach) * slope
        us = [line_ref[pl.ds(SUB + j, SUB, stride=count), :] for j in range(-3, count + 3)]
        for j, value in enumerate(line_max(us, eps, scale)):
            out_ref[pl.ds(j, SUB, stride=count), :] = value
        acc_ref[pl.ds(base, LANES), :] = out_ref[...].T
        return carry

    lax.fori_loop(0, rows // LANES, group, 0)


def y_kernel(u_ref, low_ref, high_ref, flag_ref, wind_ref, speed_ref, acc_in, acc_ref, *, sizes, eps):
    nx, nh, ny = sizes
    first = flag_ref[0:SUB] > 0.0
    last = flag_ref[SUB : 2 * SUB] > 0.0
    for xg in range(nx // SUB):

        def column(h, carry):
            def rows(y):
                return pl.ds((xg * SUB * nh + h) * ny + y, SUB, stride=nh * ny)

            center = [u_ref[rows(y), :] for y in range(ny)]

            def halo(ref, k):
                return ref[pl.ds(pl.multiple_of((k * nh + h) * nx + xg * SUB, SUB), SUB), :]

            low = [halo(low_ref, k) for k in range(3)]
            high = [halo(high_ref, k) for k in range(3)]
            low, high = edge_fix(low, center[:2], center[-2:], high, (first, last))
            speed = speed_ref[pl.ds(pl.multiple_of(h * SUB, SUB), SUB), :]
            flows = lambda y: speed + wind_ref[pl.ds(y * nx + xg * SUB, SUB), :]
            for y, value in enumerate(line_upwind(low + center + high, eps, flows)):
                acc_ref[rows(y), :] = acc_in[rows(y), :] + value
            return carry

        lax.fori_loop(0, nh, column, 0)


def head_kernel(u_ref, low_ref, high_ref, acc_in, acc_ref, *, sizes, eps, scale):
    nx, nh, ny = sizes

    def line(x, carry):
        for yg in range(ny // SUB):

            def rows(h, height=nh):
                return pl.ds(pl.multiple_of((x * height + h) * ny + yg * SUB, SUB), SUB)

            us = [low_ref[rows(k, 3), :] for k in range(3)]
            us += [u_ref[rows(h), :] for h in range(nh)]
            us += [high_ref[rows(k, 3), :] for k in range(3)]
            for h, value in enumerate(line_max(us, eps, scale)):
                acc_ref[rows(h), :] = acc_in[rows(h), :] + value
        return carry

    lax.fori_loop(0, nx, line, 0)


def x_kernel(*refs, sizes, eps, stage, swap_y):
    nx, nh, ny = sizes
    it = iter(refs)
    u_ref, low_ref, high_ref, flag_ref, wind_ref, speed_ref, acc_in, rate_ref = (next(it) for _ in range(8))
    first_ref = next(it) if stage > 1 else u_ref
    next_ref = next(it)
    first = flag_ref[2 * SUB : 3 * SUB] > 0.0
    last = flag_ref[3 * SUB : 4 * SUB] > 0.0
    step = CFL_NUMBER / rate_ref[...]

    def line(h, carry):
        for yg in range(ny // SUB):

            def rows(x):
                return pl.ds(pl.multiple_of((x * nh + h) * ny + yg * SUB, SUB), SUB)

            center = [u_ref[rows(x), :] for x in range(nx)]
            low = [low_ref[rows(k), :] for k in range(3)]
            high = [high_ref[rows(k), :] for k in range(3)]
            low, high = edge_fix(low, center[:2], center[-2:], high, (first, last))
            speed = speed_ref[pl.ds(pl.multiple_of(h * SUB, SUB), SUB), :]
            flows = lambda x: speed + wind_ref[pl.ds(x * ny + yg * SUB, SUB), :]
            for x, value in enumerate(line_upwind(low + center + high, eps, flows)):
                change = step * jnp.minimum(acc_in[rows(x), :] + value, 0.0)
                if stage == 1:
                    new = center[x] + change
                elif stage == 2:
                    new = 0.75 * first_ref[rows(x), :] + 0.25 * (center[x] + change)
                else:
                    start = first_ref[rows(x), :]
                    new = (2.0 / 3.0) * ((center[x] - start) + change)
                next_ref[rows(x), :] = new
        return carry

    lax.fori_loop(0, nh, line, 0)
    if stage < 3:
        pack_faces(next_ref, list(it), flag_ref, sizes, swap_y)


def pack_faces(u_ref, faces, flag_ref, sizes, swap_y):
    nx, nh, ny = sizes
    plane = nh * ny
    xlo, xhi, hlo, hhi = faces[:4]
    xlo[...] = u_ref[pl.ds(0, 3 * plane), :]
    xhi[...] = u_ref[pl.ds((nx - 3) * plane, 3 * plane), :]
    for x in range(nx):
        hlo[pl.ds(x * 3 * ny, 3 * ny), :] = u_ref[pl.ds(x * plane, 3 * ny), :]
        hhi[pl.ds(x * 3 * ny, 3 * ny), :] = u_ref[pl.ds(x * plane + (nh - 3) * ny, 3 * ny), :]
    first = flag_ref[0:SUB] > 0.0
    for xg in range(nx // SUB):

        def column(h, carry):
            for k in range(3):

                def rows(y):
                    return pl.ds((xg * SUB * nh + h) * ny + y, SUB, stride=plane)

                at = pl.ds(pl.multiple_of((k * nh + h) * nx + xg * SUB, SUB), SUB)
                low = u_ref[rows(k), :]
                high = u_ref[rows(ny - 3 + k), :]
                if swap_y:
                    faces[4][at, :] = jnp.where(first, high, low)
                else:
                    faces[4][at, :] = low
                    faces[5][at, :] = high
            return carry

        lax.fori_loop(0, nh, column, 0)


def pack_kernel(u_ref, flag_ref, *faces, sizes, swap_y):
    pack_faces(u_ref, list(faces), flag_ref, sizes, swap_y)


VM = pl.BlockSpec(memory_space=pltpu.VMEM)


def call(kernel, name, ins, outs, flops, scratch=()):
    shapes = [jax.ShapeDtypeStruct(s, jnp.float32) for s in outs]
    got = pl.pallas_call(
        kernel,
        out_shape=shapes,
        in_specs=[VM] * len(ins),
        out_specs=[VM] * len(outs),
        scratch_shapes=[pltpu.VMEM(s, jnp.float32) for s in scratch],
        name=name,
        cost_estimate=pl.CostEstimate(flops=flops, transcendentals=0, bytes_accessed=1024),
    )(*ins)
    return got


def neighbours(low_face, high_face, axis, closed):
    count = lax.axis_size(axis)
    ends = count if closed else count - 1
    from_low = lax.ppermute(high_face, axis, [(i, (i + 1) % count) for i in range(ends)])
    from_high = lax.ppermute(low_face, axis, [((i + 1) % count, i) for i in range(ends)])
    return from_low, from_high


def all_max(value, axes):
    for axis in axes:
        count = lax.axis_size(axis)
        if count & (count - 1):
            value = lax.pmax(value, axis)
            continue
        reach = 1
        while reach < count:
            value = jnp.maximum(
                value, lax.ppermute(value, axis, [(i, i ^ reach) for i in range(count)])
            )
            reach *= 2
    return value


def body(level_set, wind_field):
    nx, ny, nh, nv = level_set.shape
    sizes = (nx, nh, ny)
    rows = nx * nh * ny
    n_head = nh * lax.axis_size("ha")
    d_theta = 2.0 * math.pi / n_head
    d_speed = SPEED_SPAN / nv
    count_y = lax.axis_size("gy")
    swap_y = count_y == 2

    angles = np.arange(n_head) * d_theta
    cosines, sines = np.cos(angles), np.sin(angles)
    speeds = SPEED_LOW + SPEED_SPAN * (np.arange(nv) + 0.5) / nv

    def edge(axis, at):
        return (lax.axis_index(axis) == at).astype(jnp.float32)

    flags = jnp.stack(
        [edge("gy", 0), edge("gy", count_y - 1), edge("gx", 0), edge("gx", lax.axis_size("gx") - 1)]
    )
    flags = jnp.broadcast_to(flags[:, None, None], (4, SUB, nv)).reshape(4 * SUB, nv)

    ends = np.array([speeds[0], speeds[-1]])
    cos_ends = jnp.asarray((ends[:, None] * cosines).reshape(-1, 1, 1), jnp.float32)
    sin_ends = jnp.asarray((ends[:, None] * sines).reshape(-1, 1, 1), jnp.float32)
    top = jnp.max(
        jnp.abs(cos_ends + wind_field[0]) / CELL_SIZE + jnp.abs(sin_ends + wind_field[1]) / CELL_SIZE
    )
    top = jnp.broadcast_to(top + (TURN_MAX / d_theta + ACCEL_MAX / d_speed), (SUB, nv))

    head = lax.axis_index("ha") * nh

    def flow_rows(table):
        full = jnp.asarray(table[:, None] * speeds / CELL_SIZE, jnp.float32)
        mine = lax.dynamic_slice_in_dim(full, head, nh, 0)
        return jnp.broadcast_to(mine[:, None, :], (nh, SUB, nv)).reshape(nh * SUB, nv)

    speed_x, speed_y = flow_rows(cosines), flow_rows(sines)
    wind = wind_field * (1.0 / CELL_SIZE)
    wind_x = jnp.broadcast_to(wind[0][:, :, None], (nx, ny, nv)).reshape(nx * ny, nv)
    wind_y = jnp.broadcast_to(wind[1].T[:, :, None], (ny, nx, nv)).reshape(ny * nx, nv)

    start = level_set.transpose(0, 2, 1, 3).reshape(rows, nv)
    x_face, h_face, y_face = (3 * nh * ny, nv), (nx * 3 * ny, nv), (3 * nh * nx, nv)
    face_shapes = [x_face, x_face, h_face, h_face] + [y_face] * (1 if swap_y else 2)
    vregs = rows // SUB
    flops = vregs * 40 * SUB * LANES

    eps_g = 0.75 * WENO_EPS * CELL_SIZE**2
    eps_h = 0.75 * WENO_EPS * d_theta**2
    eps_v = 0.75 * WENO_EPS * d_speed**2

    faces = call(
        functools.partial(pack_kernel, sizes=sizes, swap_y=swap_y), "pack", [start, flags], face_shapes, 1000
    )
    rate = all_max(top, ("gy", "gx"))
    u = start
    for stage in (1, 2, 3):
        from_xl, from_xh = neighbours(faces[0], faces[1], "gx", False)
        from_hl, from_hh = neighbours(faces[2], faces[3], "ha", True)
        if swap_y:
            from_yl = from_yh = lax.ppermute(faces[4], "gy", [(0, 1), (1, 0)])
        else:
            from_yl, from_yh = neighbours(faces[4], faces[5], "gy", False)
        (acc,) = call(
            functools.partial(speed_kernel, eps=eps_v, scale=ACCEL_MAX / (6.0 * d_speed)),
            f"speed{stage}",
            [u],
            [(rows, nv)],
            flops,
            [(LANES + 2 * SUB, LANES), (LANES, LANES)],
        )
        (acc,) = call(
            functools.partial(y_kernel, sizes=sizes, eps=eps_g),
            f"y{stage}",
            [u, from_yl, from_yh, flags, wind_y, speed_y, acc],
            [(rows, nv)],
            flops,
        )
        (acc,) = call(
            functools.partial(head_kernel, sizes=sizes, eps=eps_h, scale=TURN_MAX / (6.0 * d_theta)),
            f"head{stage}",
            [u, from_hl, from_hh, acc],
            [(rows, nv)],
            flops,
        )
        ins = [u, from_xl, from_xh, flags, wind_x, speed_x, acc, rate]
        if stage > 1:
            ins.append(start)
        got = call(
            functools.partial(x_kernel, sizes=sizes, eps=eps_g, stage=stage, swap_y=swap_y),
            f"x{stage}",
            ins,
            [(rows, nv)] + (face_shapes if stage < 3 else []),
            flops,
        )
        u, faces = got[0], got[1:]
    return u.reshape(nx, nh, ny, nv).transpose(0, 2, 1, 3)


def solution(mesh):
    return jax.shard_map(
        body,
        mesh=mesh,
        in_specs=(P("gx", "gy", "ha", None), P(None, "gx", "gy")),
        out_specs=P("gx", "gy", "ha", None),
        check_vma=False,
    )
```

```python
import functools
import math

import jax
import jax.numpy as jnp
import numpy as np
from jax import lax
from jax.experimental import pallas as pl
from jax.experimental.pallas import tpu as pltpu
from jax.sharding import PartitionSpec as P

CELL_SIZE = 0.05
SPEED_LOW = 0.1
SPEED_SPAN = 0.4
TURN_MAX = 1.0
ACCEL_MAX = 0.05
CFL_NUMBER = 0.5
WENO_EPS = 1e-06
SUB = 8
LANES = 128


def weno_terms(us, eps):
    n = len(us) - 6
    u = {i - 3: v for i, v in enumerate(us)}
    q = {r: u[r] - u[r - 1] for r in range(-2, n + 3)}
    p = {m: q[m + 1] - q[m] for m in range(-2, n + 2)}
    t, alpha, beta, gamma, a3, g3 = {}, {}, {}, {}, {}, {}
    for r in range(-1, n + 2):
        t[r] = p[r] - p[r - 1]
        z = 1.5 * t[r]
        base = t[r] * t[r] + ((0.75 * p[r - 1]) * p[r] + eps)
        if r <= n - 1:
            s = base + p[r] * z
            alpha[r] = pl.reciprocal(s * s, approx=APPROX)
            a3[r] = (1.0 / 3.0) * alpha[r]
        if r >= 1:
            s = base - p[r - 1] * z
            gamma[r] = pl.reciprocal(s * s, approx=APPROX)
            g3[r] = (1.0 / 3.0) * gamma[r]
        if 0 <= r <= n:
            beta[r] = pl.reciprocal(0.5 * (base * base), approx=APPROX)
    f = {m: t[m] - t[m + 1] for m in range(-1, n + 1)}
    f2 = {m: f[m] + f[m] for m in range(-1, n + 1)}
    return n, q, p, alpha, beta, gamma, a3, g3, f, f2


APPROX = True


def line_max(us, eps, scale):
    n, q, p, alpha, beta, gamma, a3, g3, f, f2 = weno_terms(us, eps)
    outs = []
    for i in range(n):
        er = (g3[i + 2] * f2[i + 1] + alpha[i] * f[i]) * pl.reciprocal(
            g3[i + 2] + beta[i + 1] + alpha[i], approx=APPROX
        )
        el = (a3[i - 1] * f2[i - 1] + gamma[i + 1] * f[i]) * pl.reciprocal(
            a3[i - 1] + beta[i] + gamma[i + 1], approx=APPROX
        )
        p2 = p[i] + p[i]
        right = (6.0 * q[i + 1] - p2) - (p[i + 1] + er)
        minus_left = -(6.0 * q[i] + p2) - (p[i - 1] + el)
        outs.append(scale * jnp.maximum(right, minus_left))
    return outs


def line_upwind(us, eps, flows):
    n, q, p, alpha, beta, gamma, a3, g3, f, f2 = weno_terms(us, eps)
    outs = []
    for i in range(n):
        flow = flows(i)
        right = flow > 0.0
        w1 = jnp.where(right, g3[i + 2], a3[i - 1])
        w2 = jnp.where(right, beta[i + 1], beta[i])
        w3 = jnp.where(right, alpha[i], gamma[i + 1])
        f1 = jnp.where(right, f2[i + 1], f2[i - 1])
        pn = jnp.where(right, p[i + 1], p[i - 1])
        qn = jnp.where(right, q[i + 1], q[i])
        e = (w1 * f1 + w3 * f[i]) * pl.reciprocal(w1 + w2 + w3, approx=APPROX)
        x = pn + (p[i] + p[i]) + e
        outs.append(flow * qn - jnp.abs((1.0 / 6.0) * flow) * x)
    return outs


def edge_fix(low, center_low, center_high, high, flags):
    first, last = flags
    slope = center_low[0] - center_low[1]
    low = [
        jnp.where(first, center_low[0] + reach * slope, got)
        for reach, got in zip((3.0, 2.0, 1.0), low)
    ]
    slope = center_high[1] - center_high[0]
    high = [
        jnp.where(last, center_high[1] + reach * slope, got)
        for reach, got in zip((1.0, 2.0, 3.0), high)
    ]
    return low, high


def speed_kernel(u_ref, acc_ref, line_ref, out_ref, *, eps, scale):
    rows = u_ref.shape[0]
    count = LANES // SUB

    def group(g, carry):
        base = pl.multiple_of(g * LANES, LANES)
        turned = u_ref[pl.ds(base, LANES), :].T
        line_ref[pl.ds(SUB, LANES), :] = turned
        slope = turned[0:1] - turned[1:2]
        for reach in (1, 2, 3):
            line_ref[pl.ds(SUB - reach, 1), :] = turned[0:1] + float(reach) * slope
        slope = turned[LANES - 1 :] - turned[LANES - 2 : LANES - 1]
        for reach in (1, 2, 3):
            line_ref[pl.ds(SUB + LANES - 1 + reach, 1), :] = turned[LANES - 1 :] + float(reach) * slope
        us = [line_ref[pl.ds(SUB + j, SUB, stride=count), :] for j in range(-3, count + 3)]
        for j, value in enumerate(line_max(us, eps, scale)):
            out_ref[pl.ds(j, SUB, stride=count), :] = value
        acc_ref[pl.ds(base, LANES), :] = out_ref[...].T
        return carry

    lax.fori_loop(0, rows // LANES, group, 0)


def y_kernel(u_ref, low_ref, high_ref, flag_ref, wind_ref, speed_ref, acc_in, acc_ref, *, sizes, eps):
    nx, nh, ny = sizes
    first = flag_ref[0:SUB] > 0.0
    last = flag_ref[SUB : 2 * SUB] > 0.0
    for xg in range(nx // SUB):

        def column(h, carry):
            def rows(y):
                return pl.ds((xg * SUB * nh + h) * ny + y, SUB, stride=nh * ny)

            center = [u_ref[rows(y), :] for y in range(ny)]

            def halo(ref, k):
                return ref[pl.ds(pl.multiple_of((k * nh + h) * nx + xg * SUB, SUB), SUB), :]

            low = [halo(low_ref, k) for k in range(3)]
            high = [halo(high_ref, k) for k in range(3)]
            low, high = edge_fix(low, center[:2], center[-2:], high, (first, last))
            speed = speed_ref[pl.ds(pl.multiple_of(h * SUB, SUB), SUB), :]
            flows = lambda y: speed + wind_ref[pl.ds(y * nx + xg * SUB, SUB), :]
            for y, value in enumerate(line_upwind(low + center + high, eps, flows)):
                acc_ref[rows(y), :] = acc_in[rows(y), :] + value
            return carry

        lax.fori_loop(0, nh, column, 0)


def head_kernel(u_ref, low_ref, high_ref, acc_in, acc_ref, *, sizes, eps, scale):
    nx, nh, ny = sizes

    def line(x, carry):
        for yg in range(ny // SUB):

            def rows(h, height=nh):
                return pl.ds(pl.multiple_of((x * height + h) * ny + yg * SUB, SUB), SUB)

            us = [low_ref[rows(k, 3), :] for k in range(3)]
            us += [u_ref[rows(h), :] for h in range(nh)]
            us += [high_ref[rows(k, 3), :] for k in range(3)]
            for h, value in enumerate(line_max(us, eps, scale)):
                acc_ref[rows(h), :] = acc_in[rows(h), :] + value
        return carry

    lax.fori_loop(0, nx, line, 0)


def x_kernel(*refs, sizes, eps, stage, swap_y):
    nx, nh, ny = sizes
    it = iter(refs)
    u_ref, low_ref, high_ref, flag_ref, wind_ref, speed_ref, acc_in, rate_ref = (next(it) for _ in range(8))
    first_ref = next(it) if stage > 1 else u_ref
    next_ref = next(it)
    first = flag_ref[2 * SUB : 3 * SUB] > 0.0
    last = flag_ref[3 * SUB : 4 * SUB] > 0.0
    step = CFL_NUMBER / rate_ref[...]

    def line(h, carry):
        for yg in range(ny // SUB):

            def rows(x):
                return pl.ds(pl.multiple_of((x * nh + h) * ny + yg * SUB, SUB), SUB)

            center = [u_ref[rows(x), :] for x in range(nx)]
            low = [low_ref[rows(k), :] for k in range(3)]
            high = [high_ref[rows(k), :] for k in range(3)]
            low, high = edge_fix(low, center[:2], center[-2:], high, (first, last))
            speed = speed_ref[pl.ds(pl.multiple_of(h * SUB, SUB), SUB), :]
            flows = lambda x: speed + wind_ref[pl.ds(x * ny + yg * SUB, SUB), :]
            for x, value in enumerate(line_upwind(low + center + high, eps, flows)):
                change = step * jnp.minimum(acc_in[rows(x), :] + value, 0.0)
                if stage == 1:
                    new = center[x] + change
                elif stage == 2:
                    new = 0.75 * first_ref[rows(x), :] + 0.25 * (center[x] + change)
                else:
                    start = first_ref[rows(x), :]
                    new = (2.0 / 3.0) * ((center[x] - start) + change)
                next_ref[rows(x), :] = new
        return carry

    lax.fori_loop(0, nh, line, 0)
    if stage < 3:
        pack_faces(next_ref, list(it), flag_ref, sizes, swap_y)


def pack_faces(u_ref, faces, flag_ref, sizes, swap_y):
    nx, nh, ny = sizes
    plane = nh * ny
    xlo, xhi, hlo, hhi = faces[:4]
    xlo[...] = u_ref[pl.ds(0, 3 * plane), :]
    xhi[...] = u_ref[pl.ds((nx - 3) * plane, 3 * plane), :]
    for x in range(nx):
        hlo[pl.ds(x * 3 * ny, 3 * ny), :] = u_ref[pl.ds(x * plane, 3 * ny), :]
        hhi[pl.ds(x * 3 * ny, 3 * ny), :] = u_ref[pl.ds(x * plane + (nh - 3) * ny, 3 * ny), :]
    first = flag_ref[0:SUB] > 0.0
    for xg in range(nx // SUB):

        def column(h, carry):
            for k in range(3):

                def rows(y):
                    return pl.ds((xg * SUB * nh + h) * ny + y, SUB, stride=plane)

                at = pl.ds(pl.multiple_of((k * nh + h) * nx + xg * SUB, SUB), SUB)
                low = u_ref[rows(k), :]
                high = u_ref[rows(ny - 3 + k), :]
                if swap_y:
                    faces[4][at, :] = jnp.where(first, high, low)
                else:
                    faces[4][at, :] = low
                    faces[5][at, :] = high
            return carry

        lax.fori_loop(0, nh, column, 0)


def pack_kernel(u_ref, flag_ref, *faces, sizes, swap_y):
    pack_faces(u_ref, list(faces), flag_ref, sizes, swap_y)


VMEM_LIMIT = 8 * 1024 * 1024
VM = pl.BlockSpec(memory_space=pltpu.VMEM)


def call(kernel, name, ins, outs, flops, scratch=(), keep=True):
    shapes = [pltpu.VMEM(s, jnp.float32) if keep else jax.ShapeDtypeStruct(s, jnp.float32) for s in outs]
    ins = [pltpu.with_memory_space_constraint(x, pltpu.VMEM) for x in ins]
    got = pl.pallas_call(
        kernel,
        out_shape=shapes,
        in_specs=[VM] * len(ins),
        out_specs=[VM] * len(outs),
        scratch_shapes=[pltpu.VMEM(s, jnp.float32) for s in scratch],
        name=name,
        compiler_params=pltpu.CompilerParams(vmem_limit_bytes=VMEM_LIMIT),
        cost_estimate=pl.CostEstimate(flops=flops, transcendentals=0, bytes_accessed=1024),
    )(*ins)
    return got


def neighbours(low_face, high_face, axis, closed):
    count = lax.axis_size(axis)
    ends = count if closed else count - 1
    from_low = lax.ppermute(high_face, axis, [(i, (i + 1) % count) for i in range(ends)])
    from_high = lax.ppermute(low_face, axis, [((i + 1) % count, i) for i in range(ends)])
    return from_low, from_high


def all_max(value, axes):
    for axis in axes:
        count = lax.axis_size(axis)
        if count & (count - 1):
            value = lax.pmax(value, axis)
            continue
        reach = 1
        while reach < count:
            value = jnp.maximum(
                value, lax.ppermute(value, axis, [(i, i ^ reach) for i in range(count)])
            )
            reach *= 2
    return value


def body(level_set, wind_field):
    nx, ny, nh, nv = level_set.shape
    sizes = (nx, nh, ny)
    rows = nx * nh * ny
    n_head = nh * lax.axis_size("ha")
    d_theta = 2.0 * math.pi / n_head
    d_speed = SPEED_SPAN / nv
    count_y = lax.axis_size("gy")
    swap_y = count_y == 2

    angles = np.arange(n_head) * d_theta
    cosines, sines = np.cos(angles), np.sin(angles)
    speeds = SPEED_LOW + SPEED_SPAN * (np.arange(nv) + 0.5) / nv

    def edge(axis, at):
        return (lax.axis_index(axis) == at).astype(jnp.float32)

    flags = jnp.stack(
        [edge("gy", 0), edge("gy", count_y - 1), edge("gx", 0), edge("gx", lax.axis_size("gx") - 1)]
    )
    flags = jnp.broadcast_to(flags[:, None, None], (4, SUB, nv)).reshape(4 * SUB, nv)

    ends = np.array([speeds[0], speeds[-1]])
    cos_ends = jnp.asarray((ends[:, None] * cosines).reshape(-1, 1, 1), jnp.float32)
    sin_ends = jnp.asarray((ends[:, None] * sines).reshape(-1, 1, 1), jnp.float32)
    top = jnp.max(
        jnp.abs(cos_ends + wind_field[0]) / CELL_SIZE + jnp.abs(sin_ends + wind_field[1]) / CELL_SIZE
    )
    top = jnp.broadcast_to(top + (TURN_MAX / d_theta + ACCEL_MAX / d_speed), (SUB, nv))

    head = lax.axis_index("ha") * nh

    def flow_rows(table):
        full = jnp.asarray(table[:, None] * speeds / CELL_SIZE, jnp.float32)
        mine = lax.dynamic_slice_in_dim(full, head, nh, 0)
        return jnp.broadcast_to(mine[:, None, :], (nh, SUB, nv)).reshape(nh * SUB, nv)

    speed_x, speed_y = flow_rows(cosines), flow_rows(sines)
    wind = wind_field * (1.0 / CELL_SIZE)
    wind_x = jnp.broadcast_to(wind[0][:, :, None], (nx, ny, nv)).reshape(nx * ny, nv)
    wind_y = jnp.broadcast_to(wind[1].T[:, :, None], (ny, nx, nv)).reshape(ny * nx, nv)

    start = level_set.transpose(0, 2, 1, 3).reshape(rows, nv)
    x_face, h_face, y_face = (3 * nh * ny, nv), (nx * 3 * ny, nv), (3 * nh * nx, nv)
    face_shapes = [x_face, x_face, h_face, h_face] + [y_face] * (1 if swap_y else 2)
    vregs = rows // SUB
    flops = vregs * 40 * SUB * LANES

    eps_g = 0.75 * WENO_EPS * CELL_SIZE**2
    eps_h = 0.75 * WENO_EPS * d_theta**2
    eps_v = 0.75 * WENO_EPS * d_speed**2

    faces = call(
        functools.partial(pack_kernel, sizes=sizes, swap_y=swap_y), "pack", [start, flags], face_shapes, 1000
    )
    rate = all_max(top, ("gy", "gx"))
    u = start
    for stage in (1, 2, 3):
        from_xl, from_xh = neighbours(faces[0], faces[1], "gx", False)
        from_hl, from_hh = neighbours(faces[2], faces[3], "ha", True)
        if swap_y:
            from_yl = from_yh = lax.ppermute(faces[4], "gy", [(0, 1), (1, 0)])
        else:
            from_yl, from_yh = neighbours(faces[4], faces[5], "gy", False)
        (acc,) = call(
            functools.partial(speed_kernel, eps=eps_v, scale=ACCEL_MAX / (6.0 * d_speed)),
            f"speed{stage}",
            [u],
            [(rows, nv)],
            flops,
            [(LANES + 2 * SUB, LANES), (LANES, LANES)],
        )
        (acc,) = call(
            functools.partial(y_kernel, sizes=sizes, eps=eps_g),
            f"y{stage}",
            [u, from_yl, from_yh, flags, wind_y, speed_y, acc],
            [(rows, nv)],
            flops,
        )
        (acc,) = call(
            functools.partial(head_kernel, sizes=sizes, eps=eps_h, scale=TURN_MAX / (6.0 * d_theta)),
            f"head{stage}",
            [u, from_hl, from_hh, acc],
            [(rows, nv)],
            flops,
        )
        ins = [u, from_xl, from_xh, flags, wind_x, speed_x, acc, rate]
        if stage > 1:
            ins.append(start)
        got = call(
            functools.partial(x_kernel, sizes=sizes, eps=eps_g, stage=stage, swap_y=swap_y),
            f"x{stage}",
            ins,
            [(rows, nv)] + (face_shapes if stage < 3 else []),
            flops,
            keep=stage < 3,
        )
        u, faces = got[0], got[1:]
    return u.reshape(nx, nh, ny, nv).transpose(0, 2, 1, 3)


def solution(mesh):
    return jax.shard_map(
        body,
        mesh=mesh,
        in_specs=(P("gx", "gy", "ha", None), P(None, "gx", "gy")),
        out_specs=P("gx", "gy", "ha", None),
        check_vma=False,
    )
```

```python
import functools
import math

import jax
import jax.numpy as jnp
import numpy as np
from jax import lax
from jax.experimental import pallas as pl
from jax.experimental.pallas import tpu as pltpu
from jax.sharding import PartitionSpec as P

CELL_SIZE = 0.05
SPEED_LOW = 0.1
SPEED_SPAN = 0.4
TURN_MAX = 1.0
ACCEL_MAX = 0.05
CFL_NUMBER = 0.5
WENO_EPS = 1e-06
SUB = 8
LANES = 128


def weno_terms(us, eps):
    n = len(us) - 6
    u = {i - 3: v for i, v in enumerate(us)}
    q = {r: u[r] - u[r - 1] for r in range(-2, n + 3)}
    p = {m: q[m + 1] - q[m] for m in range(-2, n + 2)}
    t, alpha, beta, gamma, a3, g3 = {}, {}, {}, {}, {}, {}
    for r in range(-1, n + 2):
        t[r] = p[r] - p[r - 1]
        z = 1.5 * t[r]
        base = t[r] * t[r] + ((0.75 * p[r - 1]) * p[r] + eps)
        if r <= n - 1:
            s = base + p[r] * z
            alpha[r] = pl.reciprocal(s * s, approx=APPROX)
            a3[r] = (1.0 / 3.0) * alpha[r]
        if r >= 1:
            s = base - p[r - 1] * z
            gamma[r] = pl.reciprocal(s * s, approx=APPROX)
            g3[r] = (1.0 / 3.0) * gamma[r]
        if 0 <= r <= n:
            beta[r] = pl.reciprocal(0.5 * (base * base), approx=APPROX)
    f = {m: t[m] - t[m + 1] for m in range(-1, n + 1)}
    f2 = {m: f[m] + f[m] for m in range(-1, n + 1)}
    return n, q, p, alpha, beta, gamma, a3, g3, f, f2


APPROX = True


def line_max(us, eps, scale):
    n, q, p, alpha, beta, gamma, a3, g3, f, f2 = weno_terms(us, eps)
    outs = []
    for i in range(n):
        er = (g3[i + 2] * f2[i + 1] + alpha[i] * f[i]) * pl.reciprocal(
            g3[i + 2] + beta[i + 1] + alpha[i], approx=APPROX
        )
        el = (a3[i - 1] * f2[i - 1] + gamma[i + 1] * f[i]) * pl.reciprocal(
            a3[i - 1] + beta[i] + gamma[i + 1], approx=APPROX
        )
        p2 = p[i] + p[i]
        right = (6.0 * q[i + 1] - p2) - (p[i + 1] + er)
        minus_left = -(6.0 * q[i] + p2) - (p[i - 1] + el)
        outs.append(scale * jnp.maximum(right, minus_left))
    return outs


def line_upwind(us, eps, flows):
    n, q, p, alpha, beta, gamma, a3, g3, f, f2 = weno_terms(us, eps)
    outs = []
    for i in range(n):
        flow = flows(i)
        right = flow > 0.0
        w1 = jnp.where(right, g3[i + 2], a3[i - 1])
        w2 = jnp.where(right, beta[i + 1], beta[i])
        w3 = jnp.where(right, alpha[i], gamma[i + 1])
        f1 = jnp.where(right, f2[i + 1], f2[i - 1])
        pn = jnp.where(right, p[i + 1], p[i - 1])
        qn = jnp.where(right, q[i + 1], q[i])
        e = (w1 * f1 + w3 * f[i]) * pl.reciprocal(w1 + w2 + w3, approx=APPROX)
        x = pn + (p[i] + p[i]) + e
        outs.append(flow * qn - jnp.abs((1.0 / 6.0) * flow) * x)
    return outs


def edge_fix(low, center_low, center_high, high, flags):
    first, last = flags
    slope = center_low[0] - center_low[1]
    low = [
        jnp.where(first, center_low[0] + reach * slope, got)
        for reach, got in zip((3.0, 2.0, 1.0), low)
    ]
    slope = center_high[1] - center_high[0]
    high = [
        jnp.where(last, center_high[1] + reach * slope, got)
        for reach, got in zip((1.0, 2.0, 3.0), high)
    ]
    return low, high


def axis_flags(flag_ref, which):
    return [flag_ref[pl.ds((3 * which + k) * SUB, SUB), :] > 0.0 for k in range(3)]


def sided(even, load, a_ref, b_ref):
    from_a, from_b = load(a_ref), load(b_ref)
    low = [jnp.where(even, b, a) for a, b in zip(from_a, from_b)]
    high = [jnp.where(even, a, b) for a, b in zip(from_a, from_b)]
    return low, high


def speed_kernel(u_ref, acc_ref, line_ref, out_ref, *, eps, scale):
    rows = u_ref.shape[0]
    count = LANES // SUB

    def group(g, carry):
        base = pl.multiple_of(g * LANES, LANES)
        turned = u_ref[pl.ds(base, LANES), :].T
        line_ref[pl.ds(SUB, LANES), :] = turned
        slope = turned[0:1] - turned[1:2]
        for reach in (1, 2, 3):
            line_ref[pl.ds(SUB - reach, 1), :] = turned[0:1] + float(reach) * slope
        slope = turned[LANES - 1 :] - turned[LANES - 2 : LANES - 1]
        for reach in (1, 2, 3):
            line_ref[pl.ds(SUB + LANES - 1 + reach, 1), :] = turned[LANES - 1 :] + float(reach) * slope
        us = [line_ref[pl.ds(SUB + j, SUB, stride=count), :] for j in range(-3, count + 3)]
        for j, value in enumerate(line_max(us, eps, scale)):
            out_ref[pl.ds(j, SUB, stride=count), :] = value
        acc_ref[pl.ds(base, LANES), :] = out_ref[...].T
        return carry

    lax.fori_loop(0, rows // LANES, group, 0)


def y_kernel(u_ref, a_ref, b_ref, flag_ref, wind_ref, speed_ref, acc_in, acc_ref, *, sizes, eps):
    nx, nh, ny = sizes
    first, last, even = axis_flags(flag_ref, 0)
    for xg in range(nx // SUB):

        def column(h, carry):
            def rows(y):
                return pl.ds((xg * SUB * nh + h) * ny + y, SUB, stride=nh * ny)

            center = [u_ref[rows(y), :] for y in range(ny)]

            def halo(ref, k):
                return ref[pl.ds(pl.multiple_of((k * nh + h) * nx + xg * SUB, SUB), SUB), :]

            low, high = sided(even, lambda ref: [halo(ref, k) for k in range(3)], a_ref, b_ref)
            low, high = edge_fix(low, center[:2], center[-2:], high, (first, last))
            speed = speed_ref[pl.ds(pl.multiple_of(h * SUB, SUB), SUB), :]
            flows = lambda y: speed + wind_ref[pl.ds(y * nx + xg * SUB, SUB), :]
            for y, value in enumerate(line_upwind(low + center + high, eps, flows)):
                acc_ref[rows(y), :] = acc_in[rows(y), :] + value
            return carry

        lax.fori_loop(0, nh, column, 0)


def head_kernel(u_ref, a_ref, b_ref, flag_ref, acc_in, acc_ref, *, sizes, eps, scale):
    nx, nh, ny = sizes
    even = axis_flags(flag_ref, 2)[2]

    def line(x, carry):
        for yg in range(ny // SUB):

            def rows(h, height=nh):
                return pl.ds(pl.multiple_of((x * height + h) * ny + yg * SUB, SUB), SUB)

            low, high = sided(even, lambda ref: [ref[rows(k, 3), :] for k in range(3)], a_ref, b_ref)
            us = low + [u_ref[rows(h), :] for h in range(nh)] + high
            for h, value in enumerate(line_max(us, eps, scale)):
                acc_ref[rows(h), :] = acc_in[rows(h), :] + value
        return carry

    lax.fori_loop(0, nx, line, 0)


def x_kernel(*refs, sizes, eps, stage):
    nx, nh, ny = sizes
    it = iter(refs)
    u_ref, a_ref, b_ref, flag_ref, wind_ref, speed_ref, acc_in, rate_ref = (next(it) for _ in range(8))
    first_ref = next(it) if stage > 1 else u_ref
    next_ref = next(it)
    first, last, even = axis_flags(flag_ref, 1)
    step = CFL_NUMBER / rate_ref[...]

    def line(h, carry):
        for yg in range(ny // SUB):

            def rows(x):
                return pl.ds(pl.multiple_of((x * nh + h) * ny + yg * SUB, SUB), SUB)

            center = [u_ref[rows(x), :] for x in range(nx)]
            low, high = sided(even, lambda ref: [ref[rows(k), :] for k in range(3)], a_ref, b_ref)
            low, high = edge_fix(low, center[:2], center[-2:], high, (first, last))
            speed = speed_ref[pl.ds(pl.multiple_of(h * SUB, SUB), SUB), :]
            flows = lambda x: speed + wind_ref[pl.ds(x * ny + yg * SUB, SUB), :]
            for x, value in enumerate(line_upwind(low + center + high, eps, flows)):
                change = step * jnp.minimum(acc_in[rows(x), :] + value, 0.0)
                if stage == 1:
                    new = center[x] + change
                elif stage == 2:
                    new = 0.75 * first_ref[rows(x), :] + 0.25 * (center[x] + change)
                else:
                    start = first_ref[rows(x), :]
                    new = (2.0 / 3.0) * ((center[x] - start) + change)
                next_ref[rows(x), :] = new
        return carry

    lax.fori_loop(0, nh, line, 0)
    if stage < 3:
        pack_faces(next_ref, list(it), flag_ref, sizes)


def pack_faces(u_ref, faces, flag_ref, sizes):
    nx, nh, ny = sizes
    plane = nh * ny
    xa, xb, ha, hb, ya = faces[:5]
    yb = faces[5] if len(faces) > 5 else None
    even = axis_flags(flag_ref, 1)[2]

    def both(a_ref, b_ref, at, low, high, even):
        a_ref[at, :] = jnp.where(even, high, low)
        if b_ref is not None:
            b_ref[at, :] = jnp.where(even, low, high)

    def x_rows(i, carry):
        at = pl.multiple_of(i * SUB, SUB)
        low = u_ref[pl.ds(at, SUB), :]
        high = u_ref[pl.ds(at + (nx - 3) * plane, SUB), :]
        both(xa, xb, pl.ds(at, SUB), low, high, even)
        return carry

    lax.fori_loop(0, 3 * plane // SUB, x_rows, 0, unroll=6)
    even_h = axis_flags(flag_ref, 2)[2]
    for x in range(nx):
        for k in range(3 * ny // SUB):
            low = u_ref[pl.ds(x * plane + k * SUB, SUB), :]
            high = u_ref[pl.ds(x * plane + (nh - 3) * ny + k * SUB, SUB), :]
            both(ha, hb, pl.ds(x * 3 * ny + k * SUB, SUB), low, high, even_h)
    even_y = axis_flags(flag_ref, 0)[2]
    for xg in range(nx // SUB):

        def column(h, carry):
            for k in range(3):

                def rows(y):
                    return pl.ds((xg * SUB * nh + h) * ny + y, SUB, stride=plane)

                at = pl.ds(pl.multiple_of((k * nh + h) * nx + xg * SUB, SUB), SUB)
                both(ya, yb, at, u_ref[rows(k), :], u_ref[rows(ny - 3 + k), :], even_y)
            return carry

        lax.fori_loop(0, nh, column, 0)


def pack_kernel(u_ref, flag_ref, *faces, sizes):
    pack_faces(u_ref, list(faces), flag_ref, sizes)


VMEM_LIMIT = 8 * 1024 * 1024
VM = pl.BlockSpec(memory_space=pltpu.VMEM)


def call(kernel, name, ins, outs, flops, scratch=(), keep=True):
    shapes = [pltpu.VMEM(s, jnp.float32) if keep else jax.ShapeDtypeStruct(s, jnp.float32) for s in outs]
    ins = [pltpu.with_memory_space_constraint(x, pltpu.VMEM) for x in ins]
    got = pl.pallas_call(
        kernel,
        out_shape=shapes,
        in_specs=[VM] * len(ins),
        out_specs=[VM] * len(outs),
        scratch_shapes=[pltpu.VMEM(s, jnp.float32) for s in scratch],
        name=name,
        compiler_params=pltpu.CompilerParams(vmem_limit_bytes=VMEM_LIMIT),
        cost_estimate=pl.CostEstimate(flops=flops, transcendentals=0, bytes_accessed=1024),
    )(*ins)
    return got


def paired(axis):
    return lax.axis_size(axis) % 2 == 0


def neighbours(face_a, face_b, axis, closed):
    count = lax.axis_size(axis)
    ends = count if closed else count - 1
    if not paired(axis):
        got_b = lax.ppermute(face_a, axis, [(i, (i + 1) % count) for i in range(ends)])
        got_a = lax.ppermute(face_b, axis, [((i + 1) % count, i) for i in range(ends)])
        return got_a, got_b

    def swap(face, start):
        pairs = []
        for i in range(start, ends, 2):
            pairs += [(i, (i + 1) % count), ((i + 1) % count, i)]
        return lax.ppermute(face, axis, pairs) if pairs else None

    got_b = swap(face_b, 1) if face_b is not None else None
    got_a = swap(face_a, 0)
    return got_a, got_a if got_b is None else got_b


def all_max(value, axes):
    for axis in axes:
        count = lax.axis_size(axis)
        if count & (count - 1):
            value = lax.pmax(value, axis)
            continue
        reach = 1
        while reach < count:
            value = jnp.maximum(
                value, lax.ppermute(value, axis, [(i, i ^ reach) for i in range(count)])
            )
            reach *= 2
    return value


def body(level_set, wind_field):
    nx, ny, nh, nv = level_set.shape
    sizes = (nx, nh, ny)
    rows = nx * nh * ny
    n_head = nh * lax.axis_size("ha")
    d_theta = 2.0 * math.pi / n_head
    d_speed = SPEED_SPAN / nv

    angles = np.arange(n_head) * d_theta
    cosines, sines = np.cos(angles), np.sin(angles)
    speeds = SPEED_LOW + SPEED_SPAN * (np.arange(nv) + 0.5) / nv

    def edge(axis, at):
        return (lax.axis_index(axis) == at).astype(jnp.float32)

    flags = []
    for axis in ("gy", "gx", "ha"):
        even = (lax.axis_index(axis) % 2 == 0) | (not paired(axis))
        flags += [edge(axis, 0), edge(axis, lax.axis_size(axis) - 1), even.astype(jnp.float32)]
    flags = jnp.stack(flags)
    flags = jnp.broadcast_to(flags[:, None, None], (9, SUB, nv)).reshape(9 * SUB, nv)

    ends = np.array([speeds[0], speeds[-1]])
    cos_ends = jnp.asarray((ends[:, None] * cosines).reshape(-1, 1, 1), jnp.float32)
    sin_ends = jnp.asarray((ends[:, None] * sines).reshape(-1, 1, 1), jnp.float32)
    top = jnp.max(
        jnp.abs(cos_ends + wind_field[0]) / CELL_SIZE + jnp.abs(sin_ends + wind_field[1]) / CELL_SIZE
    )
    top = jnp.broadcast_to(top + (TURN_MAX / d_theta + ACCEL_MAX / d_speed), (SUB, nv))

    head = lax.axis_index("ha") * nh

    def flow_rows(table):
        full = jnp.asarray(table[:, None] * speeds / CELL_SIZE, jnp.float32)
        mine = lax.dynamic_slice_in_dim(full, head, nh, 0)
        return jnp.broadcast_to(mine[:, None, :], (nh, SUB, nv)).reshape(nh * SUB, nv)

    speed_x, speed_y = flow_rows(cosines), flow_rows(sines)
    wind = wind_field * (1.0 / CELL_SIZE)
    wind_x = jnp.broadcast_to(wind[0][:, :, None], (nx, ny, nv)).reshape(nx * ny, nv)
    wind_y = jnp.broadcast_to(wind[1].T[:, :, None], (ny, nx, nv)).reshape(ny * nx, nv)

    start = level_set.transpose(0, 2, 1, 3).reshape(rows, nv)
    x_face, h_face, y_face = (3 * nh * ny, nv), (nx * 3 * ny, nv), (3 * nh * nx, nv)
    face_shapes = [x_face, x_face, h_face, h_face] + [y_face] * (1 if lax.axis_size("gy") == 2 else 2)
    vregs = rows // SUB
    flops = vregs * 40 * SUB * LANES

    eps_g = 0.75 * WENO_EPS * CELL_SIZE**2
    eps_h = 0.75 * WENO_EPS * d_theta**2
    eps_v = 0.75 * WENO_EPS * d_speed**2

    faces = call(
        functools.partial(pack_kernel, sizes=sizes), "pack", [start, flags], face_shapes, 1000
    )
    rate = all_max(top, ("gy", "gx"))
    u = start
    for stage in (1, 2, 3):
        got_x = neighbours(faces[0], faces[1], "gx", False)
        got_h = neighbours(faces[2], faces[3], "ha", True)
        got_y = neighbours(faces[4], faces[5] if len(faces) > 5 else None, "gy", False)
        (acc,) = call(
            functools.partial(speed_kernel, eps=eps_v, scale=ACCEL_MAX / (6.0 * d_speed)),
            f"speed{stage}",
            [u],
            [(rows, nv)],
            flops,
            [(LANES + 2 * SUB, LANES), (LANES, LANES)],
        )
        (acc,) = call(
            functools.partial(y_kernel, sizes=sizes, eps=eps_g),
            f"y{stage}",
            [u, *got_y, flags, wind_y, speed_y, acc],
            [(rows, nv)],
            flops,
        )
        (acc,) = call(
            functools.partial(head_kernel, sizes=sizes, eps=eps_h, scale=TURN_MAX / (6.0 * d_theta)),
            f"head{stage}",
            [u, *got_h, flags, acc],
            [(rows, nv)],
            flops,
        )
        ins = [u, *got_x, flags, wind_x, speed_x, acc, rate]
        if stage > 1:
            ins.append(start)
        got = call(
            functools.partial(x_kernel, sizes=sizes, eps=eps_g, stage=stage),
            f"x{stage}",
            ins,
            [(rows, nv)] + (face_shapes if stage < 3 else []),
            flops,
            keep=stage < 3,
        )
        u, faces = got[0], got[1:]
    return u.reshape(nx, nh, ny, nv).transpose(0, 2, 1, 3)


def solution(mesh):
    return jax.shard_map(
        body,
        mesh=mesh,
        in_specs=(P("gx", "gy", "ha", None), P(None, "gx", "gy")),
        out_specs=P("gx", "gy", "ha", None),
        check_vma=False,
    )
```

```python
import functools
import math

import jax
import jax.numpy as jnp
import numpy as np
from jax import lax
from jax.experimental import pallas as pl
from jax.experimental.pallas import tpu as pltpu
from jax.sharding import PartitionSpec as P


CELL_SIZE = 0.05
SPEED_LOW = 0.1
SPEED_SPAN = 0.4
TURN_MAX = 1.0
ACCEL_MAX = 0.05
CFL_NUMBER = 0.5
WENO_EPS = 1e-06
SUB = 8
LANES = 128


def weno_terms(us, eps):
    n = len(us) - 6
    u = {i - 3: v for i, v in enumerate(us)}
    q = {r: u[r] - u[r - 1] for r in range(-2, n + 3)}
    p = {m: q[m + 1] - q[m] for m in range(-2, n + 2)}
    t, alpha, beta, gamma, a3, g3 = {}, {}, {}, {}, {}, {}
    for r in range(-1, n + 2):
        t[r] = p[r] - p[r - 1]
        z = 1.5 * t[r]
        base = t[r] * t[r] + ((0.75 * p[r - 1]) * p[r] + eps)
        if r <= n - 1:
            s = base + p[r] * z
            alpha[r] = pl.reciprocal(s * s, approx=APPROX)
            a3[r] = (1.0 / 3.0) * alpha[r]
        if r >= 1:
            s = base - p[r - 1] * z
            gamma[r] = pl.reciprocal(s * s, approx=APPROX)
            g3[r] = (1.0 / 3.0) * gamma[r]
        if 0 <= r <= n:
            beta[r] = pl.reciprocal(0.5 * (base * base), approx=APPROX)
    f = {m: t[m] - t[m + 1] for m in range(-1, n + 1)}
    f2 = {m: f[m] + f[m] for m in range(-1, n + 1)}
    return n, q, p, alpha, beta, gamma, a3, g3, f, f2


APPROX = True


def line_max(us, eps):
    n, q, p, alpha, beta, gamma, a3, g3, f, f2 = weno_terms(us, eps)
    q6 = {r: 6.0 * q[r] for r in range(0, n + 1)}
    outs = []
    for i in range(n):
        er = (g3[i + 2] * f2[i + 1] + alpha[i] * f[i]) * pl.reciprocal(
            g3[i + 2] + beta[i + 1] + alpha[i], approx=APPROX
        )
        el = (a3[i - 1] * f2[i - 1] + gamma[i + 1] * f[i]) * pl.reciprocal(
            a3[i - 1] + beta[i] + gamma[i + 1], approx=APPROX
        )
        p2 = p[i] + p[i]
        outs.append(jnp.minimum((p2 - q6[i + 1]) + (p[i + 1] + er), (p2 + q6[i]) + (p[i - 1] + el)))
    return outs


def line_upwind(us, eps, flows):
    n, q, p, alpha, beta, gamma, a3, g3, f, f2 = weno_terms(us, eps)
    outs = []
    for i in range(n):
        flow = flows(i)
        right = flow > 0.0
        w1 = jnp.where(right, g3[i + 2], a3[i - 1])
        w2 = jnp.where(right, beta[i + 1], beta[i])
        w3 = jnp.where(right, alpha[i], gamma[i + 1])
        f1 = jnp.where(right, f2[i + 1], f2[i - 1])
        pn = jnp.where(right, p[i + 1], p[i - 1])
        qn = jnp.where(right, q[i + 1], q[i])
        e = (w1 * f1 + w3 * f[i]) * pl.reciprocal(w1 + w2 + w3, approx=APPROX)
        x = pn + (p[i] + p[i]) + e
        outs.append(flow * qn - jnp.abs((1.0 / 6.0) * flow) * x)
    return outs


def edge_fix(low, center_low, center_high, high, flags):
    first, last = flags
    slope = center_low[0] - center_low[1]
    low = [
        jnp.where(first, center_low[0] + reach * slope, got)
        for reach, got in zip((3.0, 2.0, 1.0), low)
    ]
    slope = center_high[1] - center_high[0]
    high = [
        jnp.where(last, center_high[1] + reach * slope, got)
        for reach, got in zip((1.0, 2.0, 3.0), high)
    ]
    return low, high


def axis_flags(axis):
    count = lax.axis_size(axis)
    at = jnp.full((SUB, LANES), lax.axis_index(axis), jnp.int32)
    even = at % 2 == 0 if paired(axis) else at >= 0
    return at == 0, at == count - 1, even


def sided(even, load, a_ref, b_ref):
    from_a, from_b = load(a_ref), load(b_ref)
    low = [jnp.where(even, b, a) for a, b in zip(from_a, from_b)]
    high = [jnp.where(even, a, b) for a, b in zip(from_a, from_b)]
    return low, high


def pitch(sizes):
    _, nh, ny = sizes
    rows = nh * ny
    while rows % 8 != 4:
        rows += 1
    return rows


BLOCK = LANES // SUB
TURNED = BLOCK + 2 * SUB + 4
TERMS = BLOCK + 4


def turn(u_ref, turned_ref, h, sizes):
    nx, _, ny = sizes
    p = pitch(sizes)
    planes = nx * ny // LANES
    per = LANES // ny
    for g in range(planes):
        mat = jnp.concatenate([u_ref[pl.ds((g * per + x) * p + h * ny, ny), :] for x in range(per)], axis=0)
        mat = mat.T
        tiles = [mat[SUB * i : SUB * (i + 1)] for i in range(LANES // SUB)]
        row = lax.broadcasted_iota(jnp.int32, (SUB, LANES), 0).astype(jnp.float32)
        edge, inner = mat[0:1], mat[1:2]
        below = edge + (float(SUB) - row) * (edge - inner)
        edge, inner = mat[LANES - 1 :], mat[LANES - 2 : LANES - 1]
        above = edge + (row + 1.0) * (edge - inner)
        tiles = [below] + tiles + [above]
        base = (h * planes + g) * SUB * TURNED
        for s in range(SUB):
            for k in range(BLOCK // SUB + 2):
                turned_ref[pl.ds(base + s * TURNED + k * SUB, SUB), :] = tiles[s * (BLOCK // SUB) + k]


def speed_kernel(turned_ref, out_ref, *, eps, scale):
    groups = turned_ref.shape[0] // (SUB * TURNED)

    def group(g, carry):
        start = g * SUB * TURNED + SUB - 3
        us = [turned_ref[pl.ds(start + j, SUB, stride=TURNED), :] for j in range(BLOCK + 6)]
        for j, value in enumerate(line_max(us, eps)):
            out_ref[pl.ds(g * SUB * TERMS + j, SUB, stride=TERMS), :] = -scale * value
        return carry

    lax.fori_loop(0, groups, group, 0)


def y_kernel(u_ref, a_ref, b_ref, wind_ref, speed_ref, acc_ref, *, sizes, eps):
    nx, nh, ny = sizes
    p = pitch(sizes)
    first, last, even = axis_flags("gy")
    head = lax.axis_index("ha") * nh
    for xg in range(nx // SUB):

        def column(h, carry):
            def rows(y):
                return pl.ds(xg * SUB * p + h * ny + y, SUB, stride=p)

            center = [u_ref[rows(y), :] for y in range(ny)]

            def halo(ref, k):
                return ref[pl.ds(pl.multiple_of((k * nh + h) * nx + xg * SUB, SUB), SUB), :]

            low, high = sided(even, lambda ref: [halo(ref, k) for k in range(3)], a_ref, b_ref)
            low, high = edge_fix(low, center[:2], center[-2:], high, (first, last))
            speed = speed_ref[pl.ds(head + h, 1), :]
            flows = lambda y: speed + wind_ref[pl.ds(y * nx + xg * SUB, SUB), :]
            for y, value in enumerate(line_upwind(low + center + high, eps, flows)):
                acc_ref[rows(y), :] = value
            return carry

        lax.fori_loop(0, nh, column, 0)


def head_kernel(u_ref, a_ref, b_ref, acc_in, acc_ref, *, sizes, eps, scale):
    nx, nh, ny = sizes
    p = pitch(sizes)
    even = axis_flags("ha")[2]

    def line(x, carry):
        for yg in range(ny // SUB):

            def face(k):
                return pl.ds(pl.multiple_of((x * 3 + k) * ny + yg * SUB, SUB), SUB)

            def rows(h):
                return pl.ds(x * p + h * ny + yg * SUB, SUB)

            low, high = sided(even, lambda ref: [ref[face(k), :] for k in range(3)], a_ref, b_ref)
            us = low + [u_ref[rows(h), :] for h in range(nh)] + high
            for h, value in enumerate(line_max(us, eps)):
                acc_ref[rows(h), :] = acc_in[rows(h), :] - scale * value
        return carry

    lax.fori_loop(0, nx, line, 0)


def x_kernel(*refs, sizes, eps, stage):
    nx, nh, ny = sizes
    p = pitch(sizes)
    it = iter(refs)
    u_ref, a_ref, b_ref, wind_ref, speed_ref, acc_in, terms_ref, rate_ref = (next(it) for _ in range(8))
    first_ref = next(it) if stage > 1 else u_ref
    next_ref = next(it)
    turned_ref = next(it) if stage < 3 else None
    first, last, even = axis_flags("gx")
    head = lax.axis_index("ha") * nh
    step = CFL_NUMBER / rate_ref[...]
    planes = nx * ny // LANES
    per = LANES // ny

    def line(h, carry):
        if stage < 3:
            turn(next_ref, turned_ref, jnp.maximum(h - 1, 0), sizes)
        terms = []
        for g in range(planes):
            base = (h * planes + g) * SUB * TERMS
            mat = jnp.concatenate([terms_ref[pl.ds(base + s * TERMS, BLOCK), :] for s in range(SUB)], axis=0)
            terms.append(mat.T)
        speed = speed_ref[pl.ds(head + h, 1), :]
        for yg in range(ny // SUB):

            def rows(x):
                return pl.ds(x * p + h * ny + yg * SUB, SUB)

            def face(k):
                return pl.ds(pl.multiple_of((k * nh + h) * ny + yg * SUB, SUB), SUB)

            center = [u_ref[rows(x), :] for x in range(nx)]
            low, high = sided(even, lambda ref: [ref[face(k), :] for k in range(3)], a_ref, b_ref)
            low, high = edge_fix(low, center[:2], center[-2:], high, (first, last))
            flows = lambda x: speed + wind_ref[pl.ds(x * ny + yg * SUB, SUB), :]
            for x, value in enumerate(line_upwind(low + center + high, eps, flows)):
                at = (x % per) * ny + yg * SUB
                total = (acc_in[rows(x), :] + terms[x // per][at : at + SUB]) + value
                change = step * jnp.minimum(total, 0.0)
                if stage == 1:
                    new = center[x] + change
                elif stage == 2:
                    new = 0.75 * first_ref[rows(x), :] + 0.25 * (center[x] + change)
                else:
                    start = first_ref[rows(x), :]
                    new = (2.0 / 3.0) * ((center[x] - start) + change)
                if stage < 3:
                    next_ref[rows(x), :] = new
                else:
                    out = pl.ds(pl.multiple_of((x * nh + h) * ny + yg * SUB, SUB), SUB)
                    next_ref[out, :] = new
        return carry

    lax.fori_loop(0, nh, line, 0)
    if stage < 3:
        turn(next_ref, turned_ref, nh - 1, sizes)
        pack_faces(next_ref, list(it), sizes)


def pack_faces(u_ref, faces, sizes):
    nx, nh, ny = sizes
    p = pitch(sizes)
    xa, xb, ha, hb, ya = faces[:5]
    yb = faces[5] if len(faces) > 5 else None
    even = axis_flags("gx")[2]

    def both(a_ref, b_ref, at, low, high, even):
        a_ref[at, :] = jnp.where(even, high, low)
        if b_ref is not None:
            b_ref[at, :] = jnp.where(even, low, high)

    for k in range(3):
        for i in range(nh * ny // SUB):
            low = u_ref[pl.ds(k * p + i * SUB, SUB), :]
            high = u_ref[pl.ds((nx - 3 + k) * p + i * SUB, SUB), :]
            both(xa, xb, pl.ds(k * nh * ny + i * SUB, SUB), low, high, even)
    even_h = axis_flags("ha")[2]
    for x in range(nx):
        for k in range(3 * ny // SUB):
            low = u_ref[pl.ds(x * p + k * SUB, SUB), :]
            high = u_ref[pl.ds(x * p + (nh - 3) * ny + k * SUB, SUB), :]
            both(ha, hb, pl.ds(x * 3 * ny + k * SUB, SUB), low, high, even_h)
    even_y = axis_flags("gy")[2]
    for xg in range(nx // SUB):
        for h in range(nh):
            for k in range(3):

                def rows(y):
                    return pl.ds(xg * SUB * p + h * ny + y, SUB, stride=p)

                at = pl.ds((k * nh + h) * nx + xg * SUB, SUB)
                both(ya, yb, at, u_ref[rows(k), :], u_ref[rows(ny - 3 + k), :], even_y)


def pack_kernel(start_ref, u_ref, *rest, sizes):
    nx, nh, ny = sizes
    p = pitch(sizes)
    faces, sems = list(rest[:-1]), rest[-1]
    copies = [
        pltpu.make_async_copy(
            start_ref.at[pl.ds(x * nh * ny, nh * ny), :], u_ref.at[pl.ds(x * p, nh * ny), :], sems.at[x]
        )
        for x in range(nx)
    ]
    for copy in copies:
        copy.start()
    for copy in copies:
        copy.wait()
    pack_faces(u_ref, faces, sizes)


def turn_kernel(u_ref, turned_ref, *, sizes):
    for h in range(sizes[1]):
        turn(u_ref, turned_ref, h, sizes)


VMEM_LIMIT = 8 * 1024 * 1024
VM = pl.BlockSpec(memory_space=pltpu.VMEM)


def call(kernel, ins, outs, flops, keep=True, hbm=0, scratch=()):
    shapes = [pltpu.VMEM(s, jnp.float32) if keep else jax.ShapeDtypeStruct(s, jnp.float32) for s in outs]
    ins = [pltpu.with_memory_space_constraint(x, pltpu.HBM) for x in ins[:hbm]] + [pltpu.with_memory_space_constraint(x, pltpu.VMEM) for x in ins[hbm:]]
    return pl.pallas_call(
        kernel,
        out_shape=shapes,
        in_specs=[pl.BlockSpec(memory_space=pltpu.HBM)] * hbm + [VM] * (len(ins) - hbm),
        out_specs=[VM] * len(outs),
        scratch_shapes=list(scratch),
        compiler_params=pltpu.CompilerParams(vmem_limit_bytes=VMEM_LIMIT),
        cost_estimate=pl.CostEstimate(flops=flops, transcendentals=0, bytes_accessed=1024),
    )(*ins)


def paired(axis):
    return lax.axis_size(axis) % 2 == 0


def neighbours(face_a, face_b, axis, closed):
    count = lax.axis_size(axis)
    ends = count if closed else count - 1

    def send(face, pairs):
        return lax.ppermute(face, axis, pairs)

    if not paired(axis):
        got_b = send(face_a, [(i, (i + 1) % count) for i in range(ends)])
        got_a = send(face_b, [((i + 1) % count, i) for i in range(ends)])
        return got_a, got_b

    def swap(face, start):
        pairs = []
        for i in range(start, ends, 2):
            pairs += [(i, (i + 1) % count), ((i + 1) % count, i)]
        return send(face, pairs) if pairs else None

    got_b = swap(face_b, 1) if face_b is not None else None
    got_a = swap(face_a, 0)
    return got_a, got_a if got_b is None else got_b


def all_max(value, axes):
    for axis in axes:
        count = lax.axis_size(axis)
        if count & (count - 1):
            value = lax.pmax(value, axis)
            continue
        reach = 1
        while reach < count:
            other = lax.ppermute(value, axis, [(i, i ^ reach) for i in range(count)])
            value = jnp.maximum(value, other)
            reach *= 2
    return value


def body(level_set, wind_field):
    nx, ny, nh, nv = level_set.shape
    sizes = (nx, nh, ny)
    rows = nx * nh * ny
    n_head = nh * lax.axis_size("ha")
    d_theta = 2.0 * math.pi / n_head
    d_speed = SPEED_SPAN / nv

    angles = np.arange(n_head) * d_theta
    cosines, sines = np.cos(angles), np.sin(angles)
    speeds = SPEED_LOW + SPEED_SPAN * (np.arange(nv) + 0.5) / nv
    speed_x = jnp.asarray(cosines[:, None] * speeds / CELL_SIZE, jnp.float32)
    speed_y = jnp.asarray(sines[:, None] * speeds / CELL_SIZE, jnp.float32)

    start = level_set.transpose(0, 2, 1, 3).reshape(rows, nv)
    x_face, h_face, y_face = (3 * nh * ny, nv), (nx * 3 * ny, nv), (3 * nh * nx, nv)
    face_shapes = [x_face, x_face, h_face, h_face] + [y_face] * (1 if lax.axis_size("gy") == 2 else 2)
    padded = (nx * pitch(sizes), nv)
    groups = rows // LANES
    turned_shape, terms_shape = (groups * SUB * TURNED, LANES), (groups * SUB * TERMS, LANES)
    flops = rows * LANES * 40

    eps_g = 0.75 * WENO_EPS * CELL_SIZE**2
    eps_h = 0.75 * WENO_EPS * d_theta**2
    eps_v = 0.75 * WENO_EPS * d_speed**2

    got = call(
        functools.partial(pack_kernel, sizes=sizes),
        [start],
        [padded] + face_shapes,
        1000,
        hbm=1,
        scratch=[pltpu.SemaphoreType.DMA((nx,))],
    )
    u, faces = got[0], got[1:]
    first = u

    wind_field, *faces = lax.optimization_barrier((wind_field, *faces))
    ends = np.array([speeds[0], speeds[-1]])
    cos_ends = jnp.asarray((ends[:, None] * cosines).reshape(-1, 1, 1), jnp.float32)
    sin_ends = jnp.asarray((ends[:, None] * sines).reshape(-1, 1, 1), jnp.float32)
    top = jnp.max(
        jnp.abs(cos_ends + wind_field[0]) / CELL_SIZE + jnp.abs(sin_ends + wind_field[1]) / CELL_SIZE
    )
    top = jnp.broadcast_to(top + (TURN_MAX / d_theta + ACCEL_MAX / d_speed), (SUB, nv))
    wind = wind_field * (1.0 / CELL_SIZE)
    wind_x = jnp.broadcast_to(wind[0][:, :, None], (nx, ny, nv)).reshape(nx * ny, nv)
    wind_y = jnp.broadcast_to(wind[1].T[:, :, None], (ny, nx, nv)).reshape(ny * nx, nv)

    rate = all_max(top, ("gy", "gx"))
    for stage in (1, 2, 3):
        got_x = neighbours(faces[0], faces[1], "gx", False)
        got_h = neighbours(faces[2], faces[3], "ha", True)
        got_y = neighbours(faces[4], faces[5] if len(faces) > 5 else None, "gy", False)
        if stage == 1:
            (turned,) = call(functools.partial(turn_kernel, sizes=sizes), [u], [turned_shape], 1000)
        (terms,) = call(
            functools.partial(speed_kernel, eps=eps_v, scale=ACCEL_MAX / (6.0 * d_speed)),
            [turned],
            [terms_shape],
            flops,
        )
        (acc,) = call(
            functools.partial(y_kernel, sizes=sizes, eps=eps_g), [u, *got_y, wind_y, speed_y], [padded], flops
        )
        (acc,) = call(
            functools.partial(head_kernel, sizes=sizes, eps=eps_h, scale=TURN_MAX / (6.0 * d_theta)),
            [u, *got_h, acc],
            [padded],
            flops,
        )
        ins = [u, *got_x, wind_x, speed_x, acc, terms, rate]
        if stage > 1:
            ins.append(first)
        got = call(
            functools.partial(x_kernel, sizes=sizes, eps=eps_g, stage=stage),
            ins,
            [padded, turned_shape] + face_shapes if stage < 3 else [(rows, nv)],
            flops,
            keep=stage < 3,
        )
        if stage < 3:
            u, turned, faces = got[0], got[1], got[2:]
    return got[0].reshape(nx, nh, ny, nv).transpose(0, 2, 1, 3)


def solution(mesh):
    return jax.shard_map(
        body,
        mesh=mesh,
        in_specs=(P("gx", "gy", "ha", None), P(None, "gx", "gy")),
        out_specs=P("gx", "gy", "ha", None),
        check_vma=False,
    )
```

```python
import functools
import math

import jax
import jax.numpy as jnp
import numpy as np
from jax import lax
from jax.experimental import pallas as pl
from jax.experimental.pallas import tpu as pltpu
from jax.sharding import PartitionSpec as P


CELL_SIZE = 0.05
SPEED_LOW = 0.1
SPEED_SPAN = 0.4
TURN_MAX = 1.0
ACCEL_MAX = 0.05
CFL_NUMBER = 0.5
WENO_EPS = 1e-06
SUB = 8
LANES = 128


def weno_terms(us, eps):
    n = len(us) - 6
    u = {i - 3: v for i, v in enumerate(us)}
    q = {r: u[r] - u[r - 1] for r in range(-2, n + 3)}
    p = {m: q[m + 1] - q[m] for m in range(-2, n + 2)}
    t, alpha, beta, gamma, a3, g3 = {}, {}, {}, {}, {}, {}
    for r in range(-1, n + 2):
        t[r] = p[r] - p[r - 1]
        z = 1.5 * t[r]
        base = t[r] * t[r] + ((0.75 * p[r - 1]) * p[r] + eps)
        if r <= n - 1:
            s = base + p[r] * z
            alpha[r] = pl.reciprocal(s * s, approx=APPROX)
            a3[r] = (1.0 / 3.0) * alpha[r]
        if r >= 1:
            s = base - p[r - 1] * z
            gamma[r] = pl.reciprocal(s * s, approx=APPROX)
            g3[r] = (1.0 / 3.0) * gamma[r]
        if 0 <= r <= n:
            beta[r] = pl.reciprocal(0.5 * (base * base), approx=APPROX)
    f = {m: t[m] - t[m + 1] for m in range(-1, n + 1)}
    f2 = {m: f[m] + f[m] for m in range(-1, n + 1)}
    return n, q, p, alpha, beta, gamma, a3, g3, f, f2


APPROX = True


def line_max(us, eps):
    n, q, p, alpha, beta, gamma, a3, g3, f, f2 = weno_terms(us, eps)
    q6 = {r: 6.0 * q[r] for r in range(0, n + 1)}
    outs = []
    for i in range(n):
        er = (g3[i + 2] * f2[i + 1] + alpha[i] * f[i]) * pl.reciprocal(
            g3[i + 2] + beta[i + 1] + alpha[i], approx=APPROX
        )
        el = (a3[i - 1] * f2[i - 1] + gamma[i + 1] * f[i]) * pl.reciprocal(
            a3[i - 1] + beta[i] + gamma[i + 1], approx=APPROX
        )
        p2 = p[i] + p[i]
        outs.append(jnp.minimum((p2 - q6[i + 1]) + (p[i + 1] + er), (p2 + q6[i]) + (p[i - 1] + el)))
    return outs


def line_upwind(us, eps, flows):
    n, q, p, alpha, beta, gamma, a3, g3, f, f2 = weno_terms(us, eps)
    outs = []
    for i in range(n):
        flow = flows(i)
        right = flow > 0.0
        w1 = jnp.where(right, g3[i + 2], a3[i - 1])
        w2 = jnp.where(right, beta[i + 1], beta[i])
        w3 = jnp.where(right, alpha[i], gamma[i + 1])
        f1 = jnp.where(right, f2[i + 1], f2[i - 1])
        pn = jnp.where(right, p[i + 1], p[i - 1])
        qn = jnp.where(right, q[i + 1], q[i])
        e = (w1 * f1 + w3 * f[i]) * pl.reciprocal(w1 + w2 + w3, approx=APPROX)
        x = pn + (p[i] + p[i]) + e
        outs.append(flow * qn - jnp.abs((1.0 / 6.0) * flow) * x)
    return outs


def edge_fix(low, center_low, center_high, high, flags):
    first, last = flags
    slope = center_low[0] - center_low[1]
    low = [
        jnp.where(first, center_low[0] + reach * slope, got)
        for reach, got in zip((3.0, 2.0, 1.0), low)
    ]
    slope = center_high[1] - center_high[0]
    high = [
        jnp.where(last, center_high[1] + reach * slope, got)
        for reach, got in zip((1.0, 2.0, 3.0), high)
    ]
    return low, high


def axis_flags(axis):
    count = lax.axis_size(axis)
    at = jnp.full((SUB, LANES), lax.axis_index(axis), jnp.int32)
    even = at % 2 == 0 if paired(axis) else at >= 0
    return at == 0, at == count - 1, even


def sided(even, load, a_ref, b_ref):
    from_a, from_b = load(a_ref), load(b_ref)
    low = [jnp.where(even, b, a) for a, b in zip(from_a, from_b)]
    high = [jnp.where(even, a, b) for a, b in zip(from_a, from_b)]
    return low, high


def pitch(sizes):
    _, nh, ny = sizes
    rows = nh * ny
    while rows % 8 != 4:
        rows += 1
    return rows


BLOCK = LANES // SUB
TURNED = BLOCK + 2 * SUB + 4
TERMS = BLOCK + 4


def turn(u_ref, turned_ref, h, sizes):
    nx, _, ny = sizes
    p = pitch(sizes)
    planes = nx * ny // LANES
    per = LANES // ny
    for g in range(planes):
        mat = jnp.concatenate([u_ref[pl.ds((g * per + x) * p + h * ny, ny), :] for x in range(per)], axis=0)
        mat = mat.T
        tiles = [mat[SUB * i : SUB * (i + 1)] for i in range(LANES // SUB)]
        row = lax.broadcasted_iota(jnp.int32, (SUB, LANES), 0).astype(jnp.float32)
        edge, inner = mat[0:1], mat[1:2]
        below = edge + (float(SUB) - row) * (edge - inner)
        edge, inner = mat[LANES - 1 :], mat[LANES - 2 : LANES - 1]
        above = edge + (row + 1.0) * (edge - inner)
        tiles = [below] + tiles + [above]
        base = (h * planes + g) * SUB * TURNED
        for s in range(SUB):
            for k in range(BLOCK // SUB + 2):
                turned_ref[pl.ds(base + s * TURNED + k * SUB, SUB), :] = tiles[s * (BLOCK // SUB) + k]


def speed_kernel(turned_ref, out_ref, *, eps, scale):
    groups = turned_ref.shape[0] // (SUB * TURNED)

    def group(g, carry):
        start = g * SUB * TURNED + SUB - 3
        us = [turned_ref[pl.ds(start + j, SUB, stride=TURNED), :] for j in range(BLOCK + 6)]
        for j, value in enumerate(line_max(us, eps)):
            out_ref[pl.ds(g * SUB * TERMS + j, SUB, stride=TERMS), :] = -scale * value
        return carry

    lax.fori_loop(0, groups, group, 0)


def y_kernel(u_ref, a_ref, b_ref, wind_ref, speed_ref, acc_ref, *, sizes, eps):
    nx, nh, ny = sizes
    p = pitch(sizes)
    first, last, even = axis_flags("gy")
    head = lax.axis_index("ha") * nh
    for xg in range(nx // SUB):

        def column(h, carry):
            def rows(y):
                return pl.ds(xg * SUB * p + h * ny + y, SUB, stride=p)

            center = [u_ref[rows(y), :] for y in range(ny)]

            def halo(ref, k):
                return ref[pl.ds(pl.multiple_of((k * nh + h) * nx + xg * SUB, SUB), SUB), :]

            low, high = sided(even, lambda ref: [halo(ref, k) for k in range(3)], a_ref, b_ref)
            low, high = edge_fix(low, center[:2], center[-2:], high, (first, last))
            speed = speed_ref[pl.ds(head + h, 1), :]
            flows = lambda y: speed + wind_ref[pl.ds(y * nx + xg * SUB, SUB), :]
            for y, value in enumerate(line_upwind(low + center + high, eps, flows)):
                acc_ref[rows(y), :] = value
            return carry

        lax.fori_loop(0, nh, column, 0)


def head_kernel(u_ref, a_ref, b_ref, acc_in, acc_ref, *, sizes, eps, scale):
    nx, nh, ny = sizes
    p = pitch(sizes)
    even = axis_flags("ha")[2]

    def line(x, carry):
        for yg in range(ny // SUB):

            def face(k):
                return pl.ds(pl.multiple_of((x * 3 + k) * ny + yg * SUB, SUB), SUB)

            def rows(h):
                return pl.ds(x * p + h * ny + yg * SUB, SUB)

            low, high = sided(even, lambda ref: [ref[face(k), :] for k in range(3)], a_ref, b_ref)
            us = low + [u_ref[rows(h), :] for h in range(nh)] + high
            for h, value in enumerate(line_max(us, eps)):
                acc_ref[rows(h), :] = acc_in[rows(h), :] - scale * value
        return carry

    lax.fori_loop(0, nx, line, 0)


def x_kernel(*refs, sizes, eps, stage):
    nx, nh, ny = sizes
    p = pitch(sizes)
    it = iter(refs)
    u_ref, a_ref, b_ref, wind_ref, speed_ref, acc_in, terms_ref, rate_ref = (next(it) for _ in range(8))
    first_ref = next(it) if stage > 1 else u_ref
    next_ref = next(it)
    turned_ref = next(it) if stage < 3 else None
    if stage == 3:
        done_ref, sems = next(it), next(it)

        def out_copy(h):
            at = pl.ds(pl.multiple_of(h * ny, SUB), ny)
            return pltpu.make_async_copy(done_ref.at[:, at, :], next_ref.at[:, at, :], sems.at[h])

    first, last, even = axis_flags("gx")
    head = lax.axis_index("ha") * nh
    step = CFL_NUMBER / rate_ref[...]
    planes = nx * ny // LANES
    per = LANES // ny

    def line(h, carry):
        if stage < 3:
            turn(next_ref, turned_ref, jnp.maximum(h - 1, 0), sizes)
        terms = []
        for g in range(planes):
            base = (h * planes + g) * SUB * TERMS
            mat = jnp.concatenate([terms_ref[pl.ds(base + s * TERMS, BLOCK), :] for s in range(SUB)], axis=0)
            terms.append(mat.T)
        speed = speed_ref[pl.ds(head + h, 1), :]
        for yg in range(ny // SUB):

            def rows(x):
                return pl.ds(x * p + h * ny + yg * SUB, SUB)

            def face(k):
                return pl.ds(pl.multiple_of((k * nh + h) * ny + yg * SUB, SUB), SUB)

            center = [u_ref[rows(x), :] for x in range(nx)]
            low, high = sided(even, lambda ref: [ref[face(k), :] for k in range(3)], a_ref, b_ref)
            low, high = edge_fix(low, center[:2], center[-2:], high, (first, last))
            flows = lambda x: speed + wind_ref[pl.ds(x * ny + yg * SUB, SUB), :]
            for x, value in enumerate(line_upwind(low + center + high, eps, flows)):
                at = (x % per) * ny + yg * SUB
                total = (acc_in[rows(x), :] + terms[x // per][at : at + SUB]) + value
                change = step * jnp.minimum(total, 0.0)
                if stage == 1:
                    new = center[x] + change
                elif stage == 2:
                    new = 0.75 * first_ref[rows(x), :] + 0.25 * (center[x] + change)
                else:
                    start = first_ref[rows(x), :]
                    new = (2.0 / 3.0) * ((center[x] - start) + change)
                if stage < 3:
                    next_ref[rows(x), :] = new
                else:
                    done_ref[x, pl.ds(pl.multiple_of(h * ny + yg * SUB, SUB), SUB), :] = new
        if stage == 3:
            out_copy(h).start()
        return carry

    lax.fori_loop(0, nh, line, 0)
    if stage == 3:
        for h in range(nh):
            out_copy(h).wait()
        return
    turn(next_ref, turned_ref, nh - 1, sizes)
    pack_faces(next_ref, list(it), sizes)


def pack_faces(u_ref, faces, sizes):
    nx, nh, ny = sizes
    p = pitch(sizes)
    xa, xb, ha, hb = faces[:4]
    even = axis_flags("gx")[2]
    for k in range(3):
        for i in range(nh * ny // SUB):
            low = u_ref[pl.ds(k * p + i * SUB, SUB), :]
            high = u_ref[pl.ds((nx - 3 + k) * p + i * SUB, SUB), :]
            both(xa, xb, pl.ds(k * nh * ny + i * SUB, SUB), low, high, even)
    even_h = axis_flags("ha")[2]
    for x in range(nx):
        for k in range(3 * ny // SUB):
            low = u_ref[pl.ds(x * p + k * SUB, SUB), :]
            high = u_ref[pl.ds(x * p + (nh - 3) * ny + k * SUB, SUB), :]
            both(ha, hb, pl.ds(x * 3 * ny + k * SUB, SUB), low, high, even_h)
    y_faces(u_ref, faces[4:], sizes)


def both(a_ref, b_ref, at, low, high, even):
    a_ref[at, :] = jnp.where(even, high, low)
    if b_ref is not None:
        b_ref[at, :] = jnp.where(even, low, high)


def y_faces(u_ref, faces, sizes):
    nx, nh, ny = sizes
    p = pitch(sizes)
    ya, yb = faces[0], faces[1] if len(faces) > 1 else None
    even_y = axis_flags("gy")[2]
    for xg in range(nx // SUB):
        for h in range(nh):
            for k in range(3):

                def rows(y):
                    return pl.ds(xg * SUB * p + h * ny + y, SUB, stride=p)

                at = pl.ds((k * nh + h) * nx + xg * SUB, SUB)
                both(ya, yb, at, u_ref[rows(k), :], u_ref[rows(ny - 3 + k), :], even_y)


def pack_kernel(start_ref, wind_ref, rate_ref, xa, xb, ha, hb, wind, sems, *, sizes, ends, rest):
    nx, nh, ny = sizes
    plane, count = nh * ny, iter(range(2 * nx + 3))

    def copy(source, target):
        got = pltpu.make_async_copy(source, target, sems.at[next(count)])
        got.start()
        return got

    def side(axis, high, flip):
        even = lax.axis_index(axis) % 2 == 0 if paired(axis) else True
        return pl.multiple_of(jnp.where(jnp.logical_xor(even, flip), high, 0), SUB)

    copies = []
    for face, flip in ((hb, True), (ha, False)):
        at = side("ha", (nh - 3) * ny, flip)
        for x in range(nx):
            source = start_ref.at[pl.ds(x * plane + at, 3 * ny), :]
            copies.append(copy(source, face.at[pl.ds(x * 3 * ny, 3 * ny), :]))
    for face, flip in ((xa, False), (xb, True)):
        copies.append(copy(start_ref.at[pl.ds(side("gx", (nx - 3) * plane, flip), 3 * plane), :], face))
    copy(wind_ref, wind).wait()
    top = None
    for along_x, along_y in ends:
        rate = jnp.abs(wind[0] * (1.0 / CELL_SIZE) + along_x) + jnp.abs(wind[1] * (1.0 / CELL_SIZE) + along_y)
        top = rate if top is None else jnp.maximum(top, rate)
    rate_ref[...] = jnp.full(rate_ref.shape, jnp.max(top) + rest, jnp.float32)
    for got in copies:
        got.wait()


def prep_kernel(start_ref, wind_ref, u_ref, turned_ref, wind_x, wind_y, *refs, sizes):
    nx, nh, ny = sizes
    p = pitch(sizes)
    faces, (wind, columns, sems) = refs[:-3], refs[-3:]
    copies = [
        pltpu.make_async_copy(
            start_ref.at[pl.ds(x * nh * ny, nh * ny), :], u_ref.at[pl.ds(x * p, nh * ny), :], sems.at[x]
        )
        for x in range(nx)
    ]
    copies.append(pltpu.make_async_copy(wind_ref, wind, sems.at[nx]))
    for copy in copies:
        copy.start()
    copies[-1].wait()
    for y in range(ny):
        for k, table in enumerate((columns, wind_y)):
            column = wind[k][:, y : y + 1] * (1.0 / CELL_SIZE)
            table[pl.ds(y * nx, nx), :] = jnp.broadcast_to(column, (nx, LANES))
    for x in range(nx):
        for yg in range(ny // SUB):
            wind_x[pl.ds(x * ny + yg * SUB, SUB), :] = columns[pl.ds(yg * SUB * nx + x, SUB, stride=nx), :]
    for copy in copies[:-1]:
        copy.wait()
    y_faces(u_ref, list(faces), sizes)
    for h in range(nh):
        turn(u_ref, turned_ref, h, sizes)


VMEM_LIMIT = 8 * 1024 * 1024
VM = pl.BlockSpec(memory_space=pltpu.VMEM)


def call(kernel, ins, outs, flops, keep=True, hbm=0, scratch=()):
    shapes = [pltpu.VMEM(s, jnp.float32) if keep else jax.ShapeDtypeStruct(s, jnp.float32) for s in outs]
    ins = [pltpu.with_memory_space_constraint(x, pltpu.HBM) for x in ins[:hbm]] + [pltpu.with_memory_space_constraint(x, pltpu.VMEM) for x in ins[hbm:]]
    return pl.pallas_call(
        kernel,
        out_shape=shapes,
        in_specs=[pl.BlockSpec(memory_space=pltpu.HBM)] * hbm + [VM] * (len(ins) - hbm),
        out_specs=[VM if keep else pl.BlockSpec(memory_space=pltpu.HBM)] * len(outs),
        scratch_shapes=list(scratch),
        compiler_params=pltpu.CompilerParams(vmem_limit_bytes=VMEM_LIMIT),
        cost_estimate=pl.CostEstimate(flops=flops, transcendentals=0, bytes_accessed=1024),
    )(*ins)


def paired(axis):
    return lax.axis_size(axis) % 2 == 0


def neighbours(face_a, face_b, axis, closed):
    count = lax.axis_size(axis)
    ends = count if closed else count - 1

    def send(face, pairs):
        return lax.ppermute(face, axis, pairs)

    if not paired(axis):
        got_b = send(face_a, [(i, (i + 1) % count) for i in range(ends)])
        got_a = send(face_b, [((i + 1) % count, i) for i in range(ends)])
        return got_a, got_b

    def swap(face, start):
        pairs = []
        for i in range(start, ends, 2):
            pairs += [(i, (i + 1) % count), ((i + 1) % count, i)]
        return send(face, pairs) if pairs else None

    got_b = swap(face_b, 1) if face_b is not None else None
    got_a = swap(face_a, 0)
    return got_a, got_a if got_b is None else got_b


def all_max(value):
    rounds = []
    for axis in ("gx", "gy"):
        count = lax.axis_size(axis)
        if count & (count - 1):
            value = lax.pmax(value, axis)
        else:
            rounds += [(axis, 1 << k) for k in range(count.bit_length() - 1)]
    rounds.sort(key=lambda step: step not in (("gx", 1), ("gy", 1)))
    for axis, reach in rounds:
        other = lax.ppermute(value, axis, [(i, i ^ reach) for i in range(lax.axis_size(axis))])
        value = jnp.maximum(value, other)
    return value


def body(level_set, wind_field):
    nx, ny, nh, nv = level_set.shape
    sizes = (nx, nh, ny)
    rows = nx * nh * ny
    n_head = nh * lax.axis_size("ha")
    d_theta = 2.0 * math.pi / n_head
    d_speed = SPEED_SPAN / nv

    angles = np.arange(n_head) * d_theta
    cosines, sines = np.cos(angles), np.sin(angles)
    speeds = SPEED_LOW + SPEED_SPAN * (np.arange(nv) + 0.5) / nv
    speed_x = jnp.asarray(cosines[:, None] * speeds / CELL_SIZE, jnp.float32)
    speed_y = jnp.asarray(sines[:, None] * speeds / CELL_SIZE, jnp.float32)

    start = level_set.transpose(0, 2, 1, 3).reshape(rows, nv)
    x_face, h_face, y_face = (3 * nh * ny, nv), (nx * 3 * ny, nv), (3 * nh * nx, nv)
    face_shapes = [x_face, x_face, h_face, h_face] + [y_face] * (1 if lax.axis_size("gy") == 2 else 2)
    padded = (nx * pitch(sizes), nv)
    groups = rows // LANES
    turned_shape, terms_shape = (groups * SUB * TURNED, LANES), (groups * SUB * TERMS, LANES)
    flops = rows * LANES * 40

    eps_g = 0.75 * WENO_EPS * CELL_SIZE**2
    eps_h = 0.75 * WENO_EPS * d_theta**2
    eps_v = 0.75 * WENO_EPS * d_speed**2

    ends = [
        (float(v * c / CELL_SIZE), float(v * s / CELL_SIZE))
        for v in (speeds[0], speeds[-1])
        for c, s in zip(cosines, sines)
    ]
    copies = pltpu.SemaphoreType.DMA
    wind_shape = wind_field.shape
    rate, *faces = call(
        functools.partial(
            pack_kernel, sizes=sizes, ends=ends, rest=TURN_MAX / d_theta + ACCEL_MAX / d_speed
        ),
        [start, wind_field],
        [(SUB, nv)] + face_shapes[:4],
        1000,
        hbm=2,
        scratch=[pltpu.VMEM(wind_shape, jnp.float32), copies((2 * nx + 3,))],
    )
    u, turned, wind_x, wind_y, *y_face = call(
        functools.partial(prep_kernel, sizes=sizes),
        [start, wind_field],
        [padded, turned_shape, (nx * ny, nv), (ny * nx, nv)] + face_shapes[4:],
        1000,
        hbm=2,
        scratch=[
            pltpu.VMEM(wind_shape, jnp.float32),
            pltpu.VMEM((ny * nx, nv), jnp.float32),
            copies((nx + 1,)),
        ],
    )
    faces += y_face
    rate = all_max(rate)
    first = u
    for stage in (1, 2, 3):
        got_x = neighbours(faces[0], faces[1], "gx", False)
        got_h = neighbours(faces[2], faces[3], "ha", True)
        got_y = neighbours(faces[4], faces[5] if len(faces) > 5 else None, "gy", False)
        (terms,) = call(
            functools.partial(speed_kernel, eps=eps_v, scale=ACCEL_MAX / (6.0 * d_speed)),
            [turned],
            [terms_shape],
            flops,
        )
        (acc,) = call(
            functools.partial(y_kernel, sizes=sizes, eps=eps_g), [u, *got_y, wind_y, speed_y], [padded], flops
        )
        (acc,) = call(
            functools.partial(head_kernel, sizes=sizes, eps=eps_h, scale=TURN_MAX / (6.0 * d_theta)),
            [u, *got_h, acc],
            [padded],
            flops,
        )
        ins = [u, *got_x, wind_x, speed_x, acc, terms, rate]
        if stage > 1:
            ins.append(first)
        got = call(
            functools.partial(x_kernel, sizes=sizes, eps=eps_g, stage=stage),
            ins,
            [padded, turned_shape] + face_shapes if stage < 3 else [(nx, nh * ny, nv)],
            flops,
            keep=stage < 3,
            scratch=[] if stage < 3 else [pltpu.VMEM((nx, nh * ny, nv), jnp.float32), copies((nh,))],
        )
        if stage < 3:
            u, turned, faces = got[0], got[1], got[2:]
    return got[0].reshape(nx, nh, ny, nv).transpose(0, 2, 1, 3)


def solution(mesh):
    return jax.shard_map(
        body,
        mesh=mesh,
        in_specs=(P("gx", "gy", "ha", None), P(None, "gx", "gy")),
        out_specs=P("gx", "gy", "ha", None),
        check_vma=False,
    )
```

```python
import functools
import math

import jax
import jax.numpy as jnp
import numpy as np
from jax import lax
from jax.experimental import pallas as pl
from jax.experimental.pallas import tpu as pltpu
from jax.sharding import PartitionSpec as P


CELL_SIZE = 0.05
SPEED_LOW = 0.1
SPEED_SPAN = 0.4
TURN_MAX = 1.0
ACCEL_MAX = 0.05
CFL_NUMBER = 0.5
WENO_EPS = 1e-06
SUB = 8
LANES = 128


def weno_terms(us, eps):
    n = len(us) - 6
    u = {i - 3: v for i, v in enumerate(us)}
    q = {r: u[r] - u[r - 1] for r in range(-2, n + 3)}
    p = {m: q[m + 1] - q[m] for m in range(-2, n + 2)}
    t, alpha, beta, gamma, a3, g3 = {}, {}, {}, {}, {}, {}
    for r in range(-1, n + 2):
        t[r] = p[r] - p[r - 1]
        z = 1.5 * t[r]
        base = t[r] * t[r] + ((0.75 * p[r - 1]) * p[r] + eps)
        if r <= n - 1:
            s = base + p[r] * z
            alpha[r] = pl.reciprocal(s * s, approx=APPROX)
            a3[r] = (1.0 / 3.0) * alpha[r]
        if r >= 1:
            s = base - p[r - 1] * z
            gamma[r] = pl.reciprocal(s * s, approx=APPROX)
            g3[r] = (1.0 / 3.0) * gamma[r]
        if 0 <= r <= n:
            beta[r] = pl.reciprocal(0.5 * (base * base), approx=APPROX)
    f = {m: t[m] - t[m + 1] for m in range(-1, n + 1)}
    f2 = {m: f[m] + f[m] for m in range(-1, n + 1)}
    return n, q, p, alpha, beta, gamma, a3, g3, f, f2


APPROX = True


def line_max(us, eps):
    n, q, p, alpha, beta, gamma, a3, g3, f, f2 = weno_terms(us, eps)
    q6 = {r: 6.0 * q[r] for r in range(0, n + 1)}
    outs = []
    for i in range(n):
        er = (g3[i + 2] * f2[i + 1] + alpha[i] * f[i]) * pl.reciprocal(
            g3[i + 2] + beta[i + 1] + alpha[i], approx=APPROX
        )
        el = (a3[i - 1] * f2[i - 1] + gamma[i + 1] * f[i]) * pl.reciprocal(
            a3[i - 1] + beta[i] + gamma[i + 1], approx=APPROX
        )
        p2 = p[i] + p[i]
        outs.append(jnp.minimum((p2 - q6[i + 1]) + (p[i + 1] + er), (p2 + q6[i]) + (p[i - 1] + el)))
    return outs


def line_upwind(us, eps, flows):
    n, q, p, alpha, beta, gamma, a3, g3, f, f2 = weno_terms(us, eps)
    outs = []
    for i in range(n):
        flow = flows(i)
        right = flow > 0.0
        w1 = jnp.where(right, g3[i + 2], a3[i - 1])
        w2 = jnp.where(right, beta[i + 1], beta[i])
        w3 = jnp.where(right, alpha[i], gamma[i + 1])
        f1 = jnp.where(right, f2[i + 1], f2[i - 1])
        pn = jnp.where(right, p[i + 1], p[i - 1])
        qn = jnp.where(right, q[i + 1], q[i])
        e = (w1 * f1 + w3 * f[i]) * pl.reciprocal(w1 + w2 + w3, approx=APPROX)
        x = pn + (p[i] + p[i]) + e
        outs.append(flow * qn - jnp.abs((1.0 / 6.0) * flow) * x)
    return outs


def edge_fix(low, center_low, center_high, high, flags):
    first, last = flags
    slope = center_low[0] - center_low[1]
    low = [
        jnp.where(first, center_low[0] + reach * slope, got)
        for reach, got in zip((3.0, 2.0, 1.0), low)
    ]
    slope = center_high[1] - center_high[0]
    high = [
        jnp.where(last, center_high[1] + reach * slope, got)
        for reach, got in zip((1.0, 2.0, 3.0), high)
    ]
    return low, high


def axis_flags(axis):
    count = lax.axis_size(axis)
    at = jnp.full((SUB, LANES), lax.axis_index(axis), jnp.int32)
    even = at % 2 == 0 if paired(axis) else at >= 0
    return at == 0, at == count - 1, even


def sided(even, load, a_ref, b_ref):
    from_a, from_b = load(a_ref), load(b_ref)
    low = [jnp.where(even, b, a) for a, b in zip(from_a, from_b)]
    high = [jnp.where(even, a, b) for a, b in zip(from_a, from_b)]
    return low, high


def pitch(sizes):
    _, nh, ny = sizes
    rows = nh * ny
    while rows % 8 != 4:
        rows += 1
    return rows


BLOCK = LANES // SUB
TURNED = BLOCK + 2 * SUB + 4
TERMS = BLOCK + 4


def turn(u_ref, turned_ref, h, sizes):
    nx, _, ny = sizes
    p = pitch(sizes)
    planes = nx * ny // LANES
    per = LANES // ny
    for g in range(planes):
        mat = jnp.concatenate([u_ref[pl.ds((g * per + x) * p + h * ny, ny), :] for x in range(per)], axis=0)
        mat = mat.T
        tiles = [mat[SUB * i : SUB * (i + 1)] for i in range(LANES // SUB)]
        row = lax.broadcasted_iota(jnp.int32, (SUB, LANES), 0).astype(jnp.float32)
        edge, inner = mat[0:1], mat[1:2]
        below = edge + (float(SUB) - row) * (edge - inner)
        edge, inner = mat[LANES - 1 :], mat[LANES - 2 : LANES - 1]
        above = edge + (row + 1.0) * (edge - inner)
        tiles = [below] + tiles + [above]
        base = (h * planes + g) * SUB * TURNED
        for s in range(SUB):
            for k in range(BLOCK // SUB + 2):
                turned_ref[pl.ds(base + s * TURNED + k * SUB, SUB), :] = tiles[s * (BLOCK // SUB) + k]


def speed_kernel(turned_ref, out_ref, *, eps, scale):
    groups = turned_ref.shape[0] // (SUB * TURNED)

    def group(g, carry):
        start = g * SUB * TURNED + SUB - 3
        us = [turned_ref[pl.ds(start + j, SUB, stride=TURNED), :] for j in range(BLOCK + 6)]
        for j, value in enumerate(line_max(us, eps)):
            out_ref[pl.ds(g * SUB * TERMS + j, SUB, stride=TERMS), :] = -scale * value
        return carry

    lax.fori_loop(0, groups, group, 0)


def y_kernel(u_ref, a_ref, b_ref, wind_ref, speed_ref, acc_ref, *, sizes, eps):
    nx, nh, ny = sizes
    p = pitch(sizes)
    first, last, even = axis_flags("gy")
    head = lax.axis_index("ha") * nh
    for xg in range(nx // SUB):

        def column(h, carry):
            def rows(y):
                return pl.ds(xg * SUB * p + h * ny + y, SUB, stride=p)

            center = [u_ref[rows(y), :] for y in range(ny)]

            def halo(ref, k):
                return ref[pl.ds(pl.multiple_of((k * nh + h) * nx + xg * SUB, SUB), SUB), :]

            low, high = sided(even, lambda ref: [halo(ref, k) for k in range(3)], a_ref, b_ref)
            low, high = edge_fix(low, center[:2], center[-2:], high, (first, last))
            speed = speed_ref[pl.ds(head + h, 1), :]
            flows = lambda y: speed + wind_ref[pl.ds(y * nx + xg * SUB, SUB), :]
            for y, value in enumerate(line_upwind(low + center + high, eps, flows)):
                acc_ref[rows(y), :] = value
            return carry

        lax.fori_loop(0, nh, column, 0)


def is_even(axis):
    return lax.axis_index(axis) % 2 == 0 if paired(axis) else None


def by_parity(even, up_when_even, run):
    if even is None:
        run(up_when_even)
        return
    pl.when(even)(lambda: run(up_when_even))
    pl.when(jnp.logical_not(even))(lambda: run(not up_when_even))


def end_line(center, face, up, edge=None):
    inside = list(center) if up else list(center)[::-1]
    beyond = list(face) if up else list(face)[::-1]
    if edge is not None:
        slope = inside[-1] - inside[-2]
        beyond = [jnp.where(edge, inside[-1] + reach * slope, got) for reach, got in zip((1.0, 2.0, 3.0), beyond)]
    return inside + beyond


def head_kernel(u_ref, face_ref, acc_in, acc_ref, *, sizes, eps, scale, face_a):
    nx, nh, ny = sizes
    p = pitch(sizes)
    half = nh // 2

    def run(up):
        cells = range(half, nh) if up else range(half - 1, -1, -1)

        def line(x, carry):
            for yg in range(ny // SUB):

                def face(k):
                    return pl.ds(pl.multiple_of((x * 3 + k) * ny + yg * SUB, SUB), SUB)

                def rows(h):
                    return pl.ds(x * p + h * ny + yg * SUB, SUB)

                keep = range(half - 3, nh) if up else range(half + 3)
                inside = [u_ref[rows(h), :] for h in keep]
                us = end_line(inside, [face_ref[face(k), :] for k in range(3)], up)
                for h, value in zip(cells, line_max(us, eps)):
                    acc_ref[rows(h), :] = acc_in[rows(h), :] - scale * value
            return carry

        lax.fori_loop(0, nx, line, 0)

    by_parity(is_even("ha"), face_a, run)


def edge_mask(up):
    first, last, _ = axis_flags("gx")
    return last if up else first


def x_half(center, face, edge, up, eps, flows):
    nx = len(center)
    half = nx // 2
    cells = list(range(half, nx) if up else range(half - 1, -1, -1))
    us = end_line(center[half - 3 :] if up else center[: half + 3], face, up, edge)
    turned_flows = (lambda i: flows(cells[i])) if up else (lambda i: -flows(cells[i]))
    return dict(zip(cells, line_upwind(us, eps, turned_flows)))


def x_first_kernel(u_ref, face_ref, wind_ref, speed_ref, acc_in, acc_ref, *, sizes, eps):
    nx, nh, ny = sizes
    p = pitch(sizes)
    head = lax.axis_index("ha") * nh

    def run(up):
        edge = edge_mask(up)

        def line(h, carry):
            speed = speed_ref[pl.ds(head + h, 1), :]
            for yg in range(ny // SUB):

                def rows(x):
                    return pl.ds(x * p + h * ny + yg * SUB, SUB)

                def face(k):
                    return pl.ds(pl.multiple_of((k * nh + h) * ny + yg * SUB, SUB), SUB)

                center = [u_ref[rows(x), :] for x in range(nx)]
                flows = lambda x: speed + wind_ref[pl.ds(x * ny + yg * SUB, SUB), :]
                got = x_half(center, [face_ref[face(k), :] for k in range(3)], edge, up, eps, flows)
                for x, value in got.items():
                    acc_ref[rows(x), :] = acc_in[rows(x), :] + value
            return carry

        lax.fori_loop(0, nh, line, 0)

    by_parity(is_even("gx"), True, run)


def x_kernel(*refs, sizes, eps, stage):
    nx, nh, ny = sizes
    p = pitch(sizes)
    it = iter(refs)
    u_ref, face_ref, wind_ref, speed_ref, acc_in, terms_ref, rate_ref = (next(it) for _ in range(7))
    first_ref = next(it) if stage > 1 else u_ref
    next_ref = next(it)
    turned_ref = next(it) if stage < 3 else None
    if stage == 3:
        done_ref, sems = next(it), next(it)

        def out_copy(h):
            at = pl.ds(pl.multiple_of(h * ny, SUB), ny)
            return pltpu.make_async_copy(done_ref.at[:, at, :], next_ref.at[:, at, :], sems.at[h])

    head = lax.axis_index("ha") * nh
    step = CFL_NUMBER / rate_ref[...]
    planes = nx * ny // LANES
    per = LANES // ny

    def run(up):
        edge = edge_mask(up)

        def line(h, carry):
            if stage < 3:
                turn(next_ref, turned_ref, jnp.maximum(h - 1, 0), sizes)
            terms = []
            for g in range(planes):
                base = (h * planes + g) * SUB * TERMS
                mat = jnp.concatenate([terms_ref[pl.ds(base + s * TERMS, BLOCK), :] for s in range(SUB)], axis=0)
                terms.append(mat.T)
            speed = speed_ref[pl.ds(head + h, 1), :]
            for yg in range(ny // SUB):

                def rows(x):
                    return pl.ds(x * p + h * ny + yg * SUB, SUB)

                def face(k):
                    return pl.ds(pl.multiple_of((k * nh + h) * ny + yg * SUB, SUB), SUB)

                center = [u_ref[rows(x), :] for x in range(nx)]
                flows = lambda x: speed + wind_ref[pl.ds(x * ny + yg * SUB, SUB), :]
                got = x_half(center, [face_ref[face(k), :] for k in range(3)], edge, up, eps, flows)
                for x in range(nx):
                    at = (x % per) * ny + yg * SUB
                    total = acc_in[rows(x), :] + terms[x // per][at : at + SUB]
                    if x in got:
                        total = total + got[x]
                    change = step * jnp.minimum(total, 0.0)
                    if stage == 1:
                        new = center[x] + change
                    elif stage == 2:
                        new = 0.75 * first_ref[rows(x), :] + 0.25 * (center[x] + change)
                    else:
                        start = first_ref[rows(x), :]
                        new = (2.0 / 3.0) * ((center[x] - start) + change)
                    if stage < 3:
                        next_ref[rows(x), :] = new
                    else:
                        done_ref[x, pl.ds(pl.multiple_of(h * ny + yg * SUB, SUB), SUB), :] = new
            if stage == 3:
                out_copy(h).start()
            return carry

        lax.fori_loop(0, nh, line, 0)

    by_parity(is_even("gx"), False, run)
    if stage == 3:
        for h in range(nh):
            out_copy(h).wait()
        return
    turn(next_ref, turned_ref, nh - 1, sizes)
    pack_faces(next_ref, list(it), sizes)


def pack_faces(u_ref, faces, sizes):
    nx, nh, ny = sizes
    p = pitch(sizes)
    xa, xb, ha, hb = faces[:4]
    even = axis_flags("gx")[2]
    for k in range(3):
        for i in range(nh * ny // SUB):
            low = u_ref[pl.ds(k * p + i * SUB, SUB), :]
            high = u_ref[pl.ds((nx - 3 + k) * p + i * SUB, SUB), :]
            both(xa, xb, pl.ds(k * nh * ny + i * SUB, SUB), low, high, even)
    even_h = axis_flags("ha")[2]
    for x in range(nx):
        for k in range(3 * ny // SUB):
            low = u_ref[pl.ds(x * p + k * SUB, SUB), :]
            high = u_ref[pl.ds(x * p + (nh - 3) * ny + k * SUB, SUB), :]
            both(ha, hb, pl.ds(x * 3 * ny + k * SUB, SUB), low, high, even_h)
    y_faces(u_ref, faces[4:], sizes)


def both(a_ref, b_ref, at, low, high, even):
    a_ref[at, :] = jnp.where(even, high, low)
    if b_ref is not None:
        b_ref[at, :] = jnp.where(even, low, high)


def y_faces(u_ref, faces, sizes):
    nx, nh, ny = sizes
    p = pitch(sizes)
    ya, yb = faces[0], faces[1] if len(faces) > 1 else None
    even_y = axis_flags("gy")[2]
    for xg in range(nx // SUB):
        for h in range(nh):
            for k in range(3):

                def rows(y):
                    return pl.ds(xg * SUB * p + h * ny + y, SUB, stride=p)

                at = pl.ds((k * nh + h) * nx + xg * SUB, SUB)
                both(ya, yb, at, u_ref[rows(k), :], u_ref[rows(ny - 3 + k), :], even_y)


def pack_kernel(start_ref, wind_ref, rate_ref, xa, xb, ha, hb, wind, sems, *, sizes, ends, rest):
    nx, nh, ny = sizes
    plane, count = nh * ny, iter(range(2 * nx + 3))

    def copy(source, target):
        got = pltpu.make_async_copy(source, target, sems.at[next(count)])
        got.start()
        return got

    def side(axis, high, flip):
        even = lax.axis_index(axis) % 2 == 0 if paired(axis) else True
        return pl.multiple_of(jnp.where(jnp.logical_xor(even, flip), high, 0), SUB)

    copies = []
    for face, flip in ((hb, True), (ha, False)):
        at = side("ha", (nh - 3) * ny, flip)
        for x in range(nx):
            source = start_ref.at[pl.ds(x * plane + at, 3 * ny), :]
            copies.append(copy(source, face.at[pl.ds(x * 3 * ny, 3 * ny), :]))
    for face, flip in ((xa, False), (xb, True)):
        copies.append(copy(start_ref.at[pl.ds(side("gx", (nx - 3) * plane, flip), 3 * plane), :], face))
    copy(wind_ref, wind).wait()
    top = None
    for along_x, along_y in ends:
        rate = jnp.abs(wind[0] * (1.0 / CELL_SIZE) + along_x) + jnp.abs(wind[1] * (1.0 / CELL_SIZE) + along_y)
        top = rate if top is None else jnp.maximum(top, rate)
    rate_ref[...] = jnp.full(rate_ref.shape, jnp.max(top) + rest, jnp.float32)
    for got in copies:
        got.wait()


def prep_kernel(start_ref, wind_ref, u_ref, turned_ref, wind_x, wind_y, *refs, sizes):
    nx, nh, ny = sizes
    p = pitch(sizes)
    faces, (wind, columns, sems) = refs[:-3], refs[-3:]
    copies = [
        pltpu.make_async_copy(
            start_ref.at[pl.ds(x * nh * ny, nh * ny), :], u_ref.at[pl.ds(x * p, nh * ny), :], sems.at[x]
        )
        for x in range(nx)
    ]
    copies.append(pltpu.make_async_copy(wind_ref, wind, sems.at[nx]))
    for copy in copies:
        copy.start()
    copies[-1].wait()
    for y in range(ny):
        for k, table in enumerate((columns, wind_y)):
            column = wind[k][:, y : y + 1] * (1.0 / CELL_SIZE)
            table[pl.ds(y * nx, nx), :] = jnp.broadcast_to(column, (nx, LANES))
    for x in range(nx):
        for yg in range(ny // SUB):
            wind_x[pl.ds(x * ny + yg * SUB, SUB), :] = columns[pl.ds(yg * SUB * nx + x, SUB, stride=nx), :]
    for copy in copies[:-1]:
        copy.wait()
    y_faces(u_ref, list(faces), sizes)
    for h in range(nh):
        turn(u_ref, turned_ref, h, sizes)


VMEM_LIMIT = 8 * 1024 * 1024
VM = pl.BlockSpec(memory_space=pltpu.VMEM)


def call(kernel, ins, outs, flops, keep=True, hbm=0, scratch=(), aliases=None):
    shapes = [pltpu.VMEM(s, jnp.float32) if keep else jax.ShapeDtypeStruct(s, jnp.float32) for s in outs]
    ins = [pltpu.with_memory_space_constraint(x, pltpu.HBM) for x in ins[:hbm]] + [pltpu.with_memory_space_constraint(x, pltpu.VMEM) for x in ins[hbm:]]
    return pl.pallas_call(
        kernel,
        out_shape=shapes,
        in_specs=[pl.BlockSpec(memory_space=pltpu.HBM)] * hbm + [VM] * (len(ins) - hbm),
        out_specs=[VM if keep else pl.BlockSpec(memory_space=pltpu.HBM)] * len(outs),
        scratch_shapes=list(scratch),
        input_output_aliases=aliases or {},
        compiler_params=pltpu.CompilerParams(vmem_limit_bytes=VMEM_LIMIT),
        cost_estimate=pl.CostEstimate(flops=flops, transcendentals=0, bytes_accessed=1024),
    )(*ins)


def paired(axis):
    return lax.axis_size(axis) % 2 == 0


def neighbours(face_a, face_b, axis, closed):
    count = lax.axis_size(axis)
    ends = count if closed else count - 1

    def send(face, pairs):
        return lax.ppermute(face, axis, pairs)

    if not paired(axis):
        got_b = send(face_a, [(i, (i + 1) % count) for i in range(ends)])
        got_a = send(face_b, [((i + 1) % count, i) for i in range(ends)])
        return got_a, got_b

    def swap(face, start):
        pairs = []
        for i in range(start, ends, 2):
            pairs += [(i, (i + 1) % count), ((i + 1) % count, i)]
        return send(face, pairs) if pairs else None

    got_b = swap(face_b, 1) if face_b is not None else None
    got_a = swap(face_a, 0)
    return got_a, got_a if got_b is None else got_b


def all_max(value):
    rounds = []
    for axis in ("gx", "gy"):
        count = lax.axis_size(axis)
        if count & (count - 1):
            value = lax.pmax(value, axis)
        else:
            rounds += [(axis, 1 << k) for k in range(count.bit_length() - 1)]
    rounds.sort(key=lambda step: step[0] == "gy")
    for axis, reach in rounds:
        other = lax.ppermute(value, axis, [(i, i ^ reach) for i in range(lax.axis_size(axis))])
        value = jnp.maximum(value, other)
    return value


def body(level_set, wind_field):
    nx, ny, nh, nv = level_set.shape
    sizes = (nx, nh, ny)
    rows = nx * nh * ny
    n_head = nh * lax.axis_size("ha")
    d_theta = 2.0 * math.pi / n_head
    d_speed = SPEED_SPAN / nv

    angles = np.arange(n_head) * d_theta
    cosines, sines = np.cos(angles), np.sin(angles)
    speeds = SPEED_LOW + SPEED_SPAN * (np.arange(nv) + 0.5) / nv
    speed_x = jnp.asarray(cosines[:, None] * speeds / CELL_SIZE, jnp.float32)
    speed_y = jnp.asarray(sines[:, None] * speeds / CELL_SIZE, jnp.float32)

    start = level_set.transpose(0, 2, 1, 3).reshape(rows, nv)
    x_face, h_face, y_face = (3 * nh * ny, nv), (nx * 3 * ny, nv), (3 * nh * nx, nv)
    face_shapes = [x_face, x_face, h_face, h_face] + [y_face] * (1 if lax.axis_size("gy") == 2 else 2)
    padded = (nx * pitch(sizes), nv)
    groups = rows // LANES
    turned_shape, terms_shape = (groups * SUB * TURNED, LANES), (groups * SUB * TERMS, LANES)
    flops = rows * LANES * 40

    eps_g = 0.75 * WENO_EPS * CELL_SIZE**2
    eps_h = 0.75 * WENO_EPS * d_theta**2
    eps_v = 0.75 * WENO_EPS * d_speed**2

    ends = [
        (float(v * c / CELL_SIZE), float(v * s / CELL_SIZE))
        for v in (speeds[0], speeds[-1])
        for c, s in zip(cosines, sines)
    ]
    copies = pltpu.SemaphoreType.DMA
    wind_shape = wind_field.shape
    rate, *faces = call(
        functools.partial(
            pack_kernel, sizes=sizes, ends=ends, rest=TURN_MAX / d_theta + ACCEL_MAX / d_speed
        ),
        [start, wind_field],
        [(SUB, nv)] + face_shapes[:4],
        1000,
        hbm=2,
        scratch=[pltpu.VMEM(wind_shape, jnp.float32), copies((2 * nx + 3,))],
    )
    u, turned, wind_x, wind_y, *y_face = call(
        functools.partial(prep_kernel, sizes=sizes),
        [start, wind_field],
        [padded, turned_shape, (nx * ny, nv), (ny * nx, nv)] + face_shapes[4:],
        1000,
        hbm=2,
        scratch=[
            pltpu.VMEM(wind_shape, jnp.float32),
            pltpu.VMEM((ny * nx, nv), jnp.float32),
            copies((nx + 1,)),
        ],
    )
    faces += y_face
    rate = all_max(rate)
    first = u
    for stage in (1, 2, 3):
        got_x = neighbours(faces[0], faces[1], "gx", False)
        got_h = neighbours(faces[2], faces[3], "ha", True)
        got_y = neighbours(faces[4], faces[5] if len(faces) > 5 else None, "gy", False)
        (terms,) = call(
            functools.partial(speed_kernel, eps=eps_v, scale=ACCEL_MAX / (6.0 * d_speed)),
            [turned],
            [terms_shape],
            flops,
        )
        (acc,) = call(
            functools.partial(y_kernel, sizes=sizes, eps=eps_g), [u, *got_y, wind_y, speed_y], [padded], flops
        )
        (acc,) = call(
            functools.partial(x_first_kernel, sizes=sizes, eps=eps_g),
            [u, got_x[0], wind_x, speed_x, acc],
            [padded],
            flops,
            aliases={4: 0},
        )
        for face_a, got in zip((True, False), got_h):
            (acc,) = call(
                functools.partial(head_kernel, sizes=sizes, eps=eps_h, scale=TURN_MAX / (6.0 * d_theta), face_a=face_a),
                [u, got, acc],
                [padded],
                flops,
                aliases={2: 0},
            )
        ins = [u, got_x[1], wind_x, speed_x, acc, terms, rate]
        if stage > 1:
            ins.append(first)
        got = call(
            functools.partial(x_kernel, sizes=sizes, eps=eps_g, stage=stage),
            ins,
            [padded, turned_shape] + face_shapes if stage < 3 else [(nx, nh * ny, nv)],
            flops,
            keep=stage < 3,
            scratch=[] if stage < 3 else [pltpu.VMEM((nx, nh * ny, nv), jnp.float32), copies((nh,))],
        )
        if stage < 3:
            u, turned, faces = got[0], got[1], got[2:]
    return got[0].reshape(nx, nh, ny, nv).transpose(0, 2, 1, 3)


def solution(mesh):
    return jax.shard_map(
        body,
        mesh=mesh,
        in_specs=(P("gx", "gy", "ha", None), P(None, "gx", "gy")),
        out_specs=P("gx", "gy", "ha", None),
        check_vma=False,
    )
```

```python
import functools
import math

import jax
import jax.numpy as jnp
import numpy as np
from jax import lax
from jax.experimental import pallas as pl
from jax.experimental.pallas import tpu as pltpu
from jax.sharding import PartitionSpec as P


CELL_SIZE = 0.05
SPEED_LOW = 0.1
SPEED_SPAN = 0.4
TURN_MAX = 1.0
ACCEL_MAX = 0.05
CFL_NUMBER = 0.5
WENO_EPS = 1e-06
SUB = 8
LANES = 128


def weno_terms(us, eps):
    n = len(us) - 6
    u = {i - 3: v for i, v in enumerate(us)}
    q = {r: u[r] - u[r - 1] for r in range(-2, n + 3)}
    p = {m: q[m + 1] - q[m] for m in range(-2, n + 2)}
    t, alpha, beta, gamma, a3, g3 = {}, {}, {}, {}, {}, {}
    for r in range(-1, n + 2):
        t[r] = p[r] - p[r - 1]
        z = 1.5 * t[r]
        base = t[r] * t[r] + ((0.75 * p[r - 1]) * p[r] + eps)
        if r <= n - 1:
            s = base + p[r] * z
            alpha[r] = pl.reciprocal(s * s, approx=APPROX)
            a3[r] = (1.0 / 3.0) * alpha[r]
        if r >= 1:
            s = base - p[r - 1] * z
            gamma[r] = pl.reciprocal(s * s, approx=APPROX)
            g3[r] = (1.0 / 3.0) * gamma[r]
        if 0 <= r <= n:
            beta[r] = pl.reciprocal(0.5 * (base * base), approx=APPROX)
    f = {m: t[m] - t[m + 1] for m in range(-1, n + 1)}
    f2 = {m: f[m] + f[m] for m in range(-1, n + 1)}
    return n, q, p, alpha, beta, gamma, a3, g3, f, f2


APPROX = True


def line_max(us, eps):
    n, q, p, alpha, beta, gamma, a3, g3, f, f2 = weno_terms(us, eps)
    q6 = {r: 6.0 * q[r] for r in range(0, n + 1)}
    outs = []
    for i in range(n):
        er = (g3[i + 2] * f2[i + 1] + alpha[i] * f[i]) * pl.reciprocal(
            g3[i + 2] + beta[i + 1] + alpha[i], approx=APPROX
        )
        el = (a3[i - 1] * f2[i - 1] + gamma[i + 1] * f[i]) * pl.reciprocal(
            a3[i - 1] + beta[i] + gamma[i + 1], approx=APPROX
        )
        p2 = p[i] + p[i]
        outs.append(jnp.minimum((p2 - q6[i + 1]) + (p[i + 1] + er), (p2 + q6[i]) + (p[i - 1] + el)))
    return outs


def line_upwind(us, eps, flows):
    n, q, p, alpha, beta, gamma, a3, g3, f, f2 = weno_terms(us, eps)
    outs = []
    for i in range(n):
        flow = flows(i)
        right = flow > 0.0
        w1 = jnp.where(right, g3[i + 2], a3[i - 1])
        w2 = jnp.where(right, beta[i + 1], beta[i])
        w3 = jnp.where(right, alpha[i], gamma[i + 1])
        f1 = jnp.where(right, f2[i + 1], f2[i - 1])
        pn = jnp.where(right, p[i + 1], p[i - 1])
        qn = jnp.where(right, q[i + 1], q[i])
        e = (w1 * f1 + w3 * f[i]) * pl.reciprocal(w1 + w2 + w3, approx=APPROX)
        x = pn + (p[i] + p[i]) + e
        outs.append(flow * qn - jnp.abs((1.0 / 6.0) * flow) * x)
    return outs


def edge_fix(low, center_low, center_high, high, flags):
    first, last = flags
    slope = center_low[0] - center_low[1]
    low = [
        jnp.where(first, center_low[0] + reach * slope, got)
        for reach, got in zip((3.0, 2.0, 1.0), low)
    ]
    slope = center_high[1] - center_high[0]
    high = [
        jnp.where(last, center_high[1] + reach * slope, got)
        for reach, got in zip((1.0, 2.0, 3.0), high)
    ]
    return low, high


def axis_flags(axis):
    count = lax.axis_size(axis)
    at = jnp.full((SUB, LANES), lax.axis_index(axis), jnp.int32)
    even = at % 2 == 0 if paired(axis) else at >= 0
    return at == 0, at == count - 1, even


def sided(even, load, a_ref, b_ref):
    from_a, from_b = load(a_ref), load(b_ref)
    low = [jnp.where(even, b, a) for a, b in zip(from_a, from_b)]
    high = [jnp.where(even, a, b) for a, b in zip(from_a, from_b)]
    return low, high


def pitch(sizes):
    _, nh, ny = sizes
    rows = nh * ny
    while rows % 8 != 4:
        rows += 1
    return rows


BLOCK = LANES // SUB
TURNED = BLOCK + 2 * SUB + 4
TERMS = BLOCK + 4


def turn(u_ref, turned_ref, h, sizes):
    nx, _, ny = sizes
    p = pitch(sizes)
    planes = nx * ny // LANES
    per = LANES // ny
    for g in range(planes):
        mat = jnp.concatenate([u_ref[pl.ds((g * per + x) * p + h * ny, ny), :] for x in range(per)], axis=0)
        mat = mat.T
        tiles = [mat[SUB * i : SUB * (i + 1)] for i in range(LANES // SUB)]
        row = lax.broadcasted_iota(jnp.int32, (SUB, LANES), 0).astype(jnp.float32)
        edge, inner = mat[0:1], mat[1:2]
        below = edge + (float(SUB) - row) * (edge - inner)
        edge, inner = mat[LANES - 1 :], mat[LANES - 2 : LANES - 1]
        above = edge + (row + 1.0) * (edge - inner)
        tiles = [below] + tiles + [above]
        base = (h * planes + g) * SUB * TURNED
        for s in range(SUB):
            for k in range(BLOCK // SUB + 2):
                turned_ref[pl.ds(base + s * TURNED + k * SUB, SUB), :] = tiles[s * (BLOCK // SUB) + k]


def speed_kernel(turned_ref, out_ref, *, eps, scale):
    groups = turned_ref.shape[0] // (SUB * TURNED)

    def group(g, carry):
        start = g * SUB * TURNED + SUB - 3
        us = [turned_ref[pl.ds(start + j, SUB, stride=TURNED), :] for j in range(BLOCK + 6)]
        for j, value in enumerate(line_max(us, eps)):
            out_ref[pl.ds(g * SUB * TERMS + j, SUB, stride=TERMS), :] = -scale * value
        return carry

    lax.fori_loop(0, groups, group, 0)


def y_kernel(u_ref, a_ref, b_ref, wind_ref, speed_ref, acc_ref, *, sizes, eps):
    nx, nh, ny = sizes
    p = pitch(sizes)
    first, last, even = axis_flags("gy")
    head = lax.axis_index("ha") * nh
    for xg in range(nx // SUB):

        def column(h, carry):
            def rows(y):
                return pl.ds(xg * SUB * p + h * ny + y, SUB, stride=p)

            center = [u_ref[rows(y), :] for y in range(ny)]

            def halo(ref, k):
                return ref[pl.ds(pl.multiple_of((k * nh + h) * nx + xg * SUB, SUB), SUB), :]

            low, high = sided(even, lambda ref: [halo(ref, k) for k in range(3)], a_ref, b_ref)
            low, high = edge_fix(low, center[:2], center[-2:], high, (first, last))
            speed = speed_ref[pl.ds(head + h, 1), :]
            flows = lambda y: speed + wind_ref[pl.ds(y * nx + xg * SUB, SUB), :]
            for y, value in enumerate(line_upwind(low + center + high, eps, flows)):
                acc_ref[rows(y), :] = value
            return carry

        lax.fori_loop(0, nh, column, 0)


def is_even(axis):
    return lax.axis_index(axis) % 2 == 0 if paired(axis) else None


def by_parity(even, up_when_even, run):
    if even is None:
        run(up_when_even)
        return
    pl.when(even)(lambda: run(up_when_even))
    pl.when(jnp.logical_not(even))(lambda: run(not up_when_even))


def end_line(center, face, up, edge=None):
    inside = list(center) if up else list(center)[::-1]
    beyond = list(face) if up else list(face)[::-1]
    if edge is not None:
        slope = inside[-1] - inside[-2]
        beyond = [jnp.where(edge, inside[-1] + reach * slope, got) for reach, got in zip((1.0, 2.0, 3.0), beyond)]
    return inside + beyond


def head_kernel(u_ref, face_ref, acc_in, acc_ref, *, sizes, eps, scale, face_a):
    nx, nh, ny = sizes
    p = pitch(sizes)
    half = nh // 2

    def run(up):
        cells = range(half, nh) if up else range(half - 1, -1, -1)

        def line(x, carry):
            for yg in range(ny // SUB):

                def face(k):
                    return pl.ds(pl.multiple_of((x * 3 + k) * ny + yg * SUB, SUB), SUB)

                def rows(h):
                    return pl.ds(x * p + h * ny + yg * SUB, SUB)

                keep = range(half - 3, nh) if up else range(half + 3)
                inside = [u_ref[rows(h), :] for h in keep]
                us = end_line(inside, [face_ref[face(k), :] for k in range(3)], up)
                for h, value in zip(cells, line_max(us, eps)):
                    acc_ref[rows(h), :] = acc_in[rows(h), :] - scale * value
            return carry

        lax.fori_loop(0, nx, line, 0)

    by_parity(is_even("ha"), face_a, run)


def edge_mask(up):
    first, last, _ = axis_flags("gx")
    return last if up else first


def x_half(center, face, edge, up, eps, flows):
    nx = len(center)
    half = nx // 2
    cells = list(range(half, nx) if up else range(half - 1, -1, -1))
    us = end_line(center[half - 3 :] if up else center[: half + 3], face, up, edge)
    turned_flows = (lambda i: flows(cells[i])) if up else (lambda i: -flows(cells[i]))
    return dict(zip(cells, line_upwind(us, eps, turned_flows)))


def x_first_kernel(u_ref, face_ref, wind_ref, speed_ref, acc_in, acc_ref, *, sizes, eps):
    nx, nh, ny = sizes
    p = pitch(sizes)
    head = lax.axis_index("ha") * nh

    def run(up):
        edge = edge_mask(up)

        def line(h, carry):
            speed = speed_ref[pl.ds(head + h, 1), :]
            for yg in range(ny // SUB):

                def rows(x):
                    return pl.ds(x * p + h * ny + yg * SUB, SUB)

                def face(k):
                    return pl.ds(pl.multiple_of((k * nh + h) * ny + yg * SUB, SUB), SUB)

                center = [u_ref[rows(x), :] for x in range(nx)]
                flows = lambda x: speed + wind_ref[pl.ds(x * ny + yg * SUB, SUB), :]
                got = x_half(center, [face_ref[face(k), :] for k in range(3)], edge, up, eps, flows)
                for x, value in got.items():
                    acc_ref[rows(x), :] = acc_in[rows(x), :] + value
            return carry

        lax.fori_loop(0, nh, line, 0)

    by_parity(is_even("gx"), True, run)


def x_kernel(*refs, sizes, eps, stage):
    nx, nh, ny = sizes
    p = pitch(sizes)
    it = iter(refs)
    u_ref, face_ref, wind_ref, speed_ref, acc_in, terms_ref, rate_ref = (next(it) for _ in range(7))
    first_ref = next(it) if stage > 1 else u_ref
    next_ref = next(it)
    turned_ref = next(it) if stage < 3 else None
    if stage == 3:
        done_ref, sems = next(it), next(it)

        def out_copy(h):
            at = pl.ds(pl.multiple_of(h * ny, SUB), ny)
            return pltpu.make_async_copy(done_ref.at[:, at, :], next_ref.at[:, at, :], sems.at[h])

    head = lax.axis_index("ha") * nh
    step = CFL_NUMBER / rate_ref[...]
    planes = nx * ny // LANES
    per = LANES // ny

    def run(up):
        edge = edge_mask(up)

        def line(h, carry):
            if stage < 3:
                turn(next_ref, turned_ref, jnp.maximum(h - 1, 0), sizes)
            terms = []
            for g in range(planes):
                base = (h * planes + g) * SUB * TERMS
                mat = jnp.concatenate([terms_ref[pl.ds(base + s * TERMS, BLOCK), :] for s in range(SUB)], axis=0)
                terms.append(mat.T)
            speed = speed_ref[pl.ds(head + h, 1), :]
            for yg in range(ny // SUB):

                def rows(x):
                    return pl.ds(x * p + h * ny + yg * SUB, SUB)

                def face(k):
                    return pl.ds(pl.multiple_of((k * nh + h) * ny + yg * SUB, SUB), SUB)

                center = [u_ref[rows(x), :] for x in range(nx)]
                flows = lambda x: speed + wind_ref[pl.ds(x * ny + yg * SUB, SUB), :]
                got = x_half(center, [face_ref[face(k), :] for k in range(3)], edge, up, eps, flows)
                for x in range(nx):
                    at = (x % per) * ny + yg * SUB
                    total = acc_in[rows(x), :] + terms[x // per][at : at + SUB]
                    if x in got:
                        total = total + got[x]
                    change = step * jnp.minimum(total, 0.0)
                    if stage == 1:
                        new = center[x] + change
                    elif stage == 2:
                        new = 0.75 * first_ref[rows(x), :] + 0.25 * (center[x] + change)
                    else:
                        start = first_ref[rows(x), :]
                        new = (2.0 / 3.0) * ((center[x] - start) + change)
                    if stage < 3:
                        next_ref[rows(x), :] = new
                    else:
                        done_ref[x, pl.ds(pl.multiple_of(h * ny + yg * SUB, SUB), SUB), :] = new
            if stage == 3:
                out_copy(h).start()
            return carry

        lax.fori_loop(0, nh, line, 0)

    by_parity(is_even("gx"), False, run)
    if stage == 3:
        for h in range(nh):
            out_copy(h).wait()
        return
    turn(next_ref, turned_ref, nh - 1, sizes)
    pack_faces(next_ref, list(it), sizes)


def pack_faces(u_ref, faces, sizes):
    nx, nh, ny = sizes
    p = pitch(sizes)
    xa, xb, ha, hb = faces[:4]
    even = axis_flags("gx")[2]
    for k in range(3):
        for i in range(nh * ny // SUB):
            low = u_ref[pl.ds(k * p + i * SUB, SUB), :]
            high = u_ref[pl.ds((nx - 3 + k) * p + i * SUB, SUB), :]
            both(xa, xb, pl.ds(k * nh * ny + i * SUB, SUB), low, high, even)
    even_h = axis_flags("ha")[2]
    for x in range(nx):
        for k in range(3 * ny // SUB):
            low = u_ref[pl.ds(x * p + k * SUB, SUB), :]
            high = u_ref[pl.ds(x * p + (nh - 3) * ny + k * SUB, SUB), :]
            both(ha, hb, pl.ds(x * 3 * ny + k * SUB, SUB), low, high, even_h)
    y_faces(u_ref, faces[4:], sizes)


def both(a_ref, b_ref, at, low, high, even):
    a_ref[at, :] = jnp.where(even, high, low)
    if b_ref is not None:
        b_ref[at, :] = jnp.where(even, low, high)


def y_faces(u_ref, faces, sizes):
    nx, nh, ny = sizes
    p = pitch(sizes)
    ya, yb = faces[0], faces[1] if len(faces) > 1 else None
    even_y = axis_flags("gy")[2]
    for xg in range(nx // SUB):
        for h in range(nh):
            for k in range(3):

                def rows(y):
                    return pl.ds(xg * SUB * p + h * ny + y, SUB, stride=p)

                at = pl.ds((k * nh + h) * nx + xg * SUB, SUB)
                both(ya, yb, at, u_ref[rows(k), :], u_ref[rows(ny - 3 + k), :], even_y)


def pack_kernel(start_ref, wind_ref, rate_ref, xa, xb, ha, hb, wind, sems, *, sizes, ends, rest):
    nx, nh, ny = sizes
    plane, count = nh * ny, iter(range(2 * nx + 3))

    def copy(source, target):
        got = pltpu.make_async_copy(source, target, sems.at[next(count)])
        got.start()
        return got

    def side(axis, high, flip):
        even = lax.axis_index(axis) % 2 == 0 if paired(axis) else True
        return pl.multiple_of(jnp.where(jnp.logical_xor(even, flip), high, 0), SUB)

    copies = []
    for face, flip in ((hb, True), (ha, False)):
        at = side("ha", (nh - 3) * ny, flip)
        for x in range(nx):
            source = start_ref.at[pl.ds(x * plane + at, 3 * ny), :]
            copies.append(copy(source, face.at[pl.ds(x * 3 * ny, 3 * ny), :]))
    for face, flip in ((xa, False), (xb, True)):
        copies.append(copy(start_ref.at[pl.ds(side("gx", (nx - 3) * plane, flip), 3 * plane), :], face))
    copy(wind_ref, wind).wait()
    top = None
    for along_x, along_y in ends:
        rate = jnp.abs(wind[0] * (1.0 / CELL_SIZE) + along_x) + jnp.abs(wind[1] * (1.0 / CELL_SIZE) + along_y)
        top = rate if top is None else jnp.maximum(top, rate)
    rate_ref[...] = jnp.full(rate_ref.shape, jnp.max(top) + rest, jnp.float32)
    for got in copies:
        got.wait()


def prep_kernel(start_ref, wind_ref, u_ref, turned_ref, wind_x, wind_y, *refs, sizes):
    nx, nh, ny = sizes
    p = pitch(sizes)
    faces, (wind, columns, sems) = refs[:-3], refs[-3:]
    copies = [
        pltpu.make_async_copy(
            start_ref.at[pl.ds(x * nh * ny, nh * ny), :], u_ref.at[pl.ds(x * p, nh * ny), :], sems.at[x]
        )
        for x in range(nx)
    ]
    copies.append(pltpu.make_async_copy(wind_ref, wind, sems.at[nx]))
    for copy in copies:
        copy.start()
    copies[-1].wait()
    for y in range(ny):
        for k, table in enumerate((columns, wind_y)):
            column = wind[k][:, y : y + 1] * (1.0 / CELL_SIZE)
            table[pl.ds(y * nx, nx), :] = jnp.broadcast_to(column, (nx, LANES))
    for x in range(nx):
        for yg in range(ny // SUB):
            wind_x[pl.ds(x * ny + yg * SUB, SUB), :] = columns[pl.ds(yg * SUB * nx + x, SUB, stride=nx), :]
    for copy in copies[:-1]:
        copy.wait()
    y_faces(u_ref, list(faces), sizes)
    for h in range(nh):
        turn(u_ref, turned_ref, h, sizes)


VMEM_LIMIT = 8 * 1024 * 1024
VM = pl.BlockSpec(memory_space=pltpu.VMEM)


def call(kernel, ins, outs, flops, keep=True, hbm=0, scratch=(), aliases=None):
    shapes = [pltpu.VMEM(s, jnp.float32) if keep else jax.ShapeDtypeStruct(s, jnp.float32) for s in outs]
    ins = [pltpu.with_memory_space_constraint(x, pltpu.HBM) for x in ins[:hbm]] + [pltpu.with_memory_space_constraint(x, pltpu.VMEM) for x in ins[hbm:]]
    return pl.pallas_call(
        kernel,
        out_shape=shapes,
        in_specs=[pl.BlockSpec(memory_space=pltpu.HBM)] * hbm + [VM] * (len(ins) - hbm),
        out_specs=[VM if keep else pl.BlockSpec(memory_space=pltpu.HBM)] * len(outs),
        scratch_shapes=list(scratch),
        input_output_aliases=aliases or {},
        compiler_params=pltpu.CompilerParams(vmem_limit_bytes=VMEM_LIMIT),
        cost_estimate=pl.CostEstimate(flops=flops, transcendentals=0, bytes_accessed=1024),
    )(*ins)


def paired(axis):
    return lax.axis_size(axis) % 2 == 0


def neighbours(face_a, face_b, axis, closed):
    count = lax.axis_size(axis)
    ends = count if closed else count - 1

    def send(face, pairs, over=axis):
        return lax.ppermute(face, over, pairs)

    if not paired(axis):
        got_b = send(face_a, [(i, (i + 1) % count) for i in range(ends)])
        got_a = send(face_b, [((i + 1) % count, i) for i in range(ends)])
        return got_a, got_b

    def swap(face, start):
        pairs = []
        for i in range(start, ends, 2):
            pairs += [(i, (i + 1) % count), ((i + 1) % count, i)]
        alone = sorted(set(range(count)) - {i for i, _ in pairs})
        side = lax.axis_size("gy")
        if not pairs or not alone or axis != "gx" or side % 2:
            return send(face, pairs) if pairs else None
        every = [(i * side + k, j * side + k) for i, j in pairs for k in range(side)]
        every += [(i * side + k, i * side + (k ^ 1)) for i in alone for k in range(side)]
        return send(face, sorted(every), (axis, "gy"))

    got_b = swap(face_b, 1) if face_b is not None else None
    got_a = swap(face_a, 0)
    return got_a, got_a if got_b is None else got_b


def all_max(value):
    rounds = []
    for axis in ("gx", "gy"):
        count = lax.axis_size(axis)
        if count & (count - 1):
            value = lax.pmax(value, axis)
        else:
            rounds += [(axis, 1 << k) for k in range(count.bit_length() - 1)]
    rounds.sort(key=lambda step: step[0] == "gy")
    for axis, reach in rounds:
        other = lax.ppermute(value, axis, [(i, i ^ reach) for i in range(lax.axis_size(axis))])
        value = jnp.maximum(value, other)
    return value


def body(level_set, wind_field):
    nx, ny, nh, nv = level_set.shape
    sizes = (nx, nh, ny)
    rows = nx * nh * ny
    n_head = nh * lax.axis_size("ha")
    d_theta = 2.0 * math.pi / n_head
    d_speed = SPEED_SPAN / nv

    angles = np.arange(n_head) * d_theta
    cosines, sines = np.cos(angles), np.sin(angles)
    speeds = SPEED_LOW + SPEED_SPAN * (np.arange(nv) + 0.5) / nv
    speed_x = jnp.asarray(cosines[:, None] * speeds / CELL_SIZE, jnp.float32)
    speed_y = jnp.asarray(sines[:, None] * speeds / CELL_SIZE, jnp.float32)

    start = level_set.transpose(0, 2, 1, 3).reshape(rows, nv)
    x_face, h_face, y_face = (3 * nh * ny, nv), (nx * 3 * ny, nv), (3 * nh * nx, nv)
    face_shapes = [x_face, x_face, h_face, h_face] + [y_face] * (1 if lax.axis_size("gy") == 2 else 2)
    padded = (nx * pitch(sizes), nv)
    groups = rows // LANES
    turned_shape, terms_shape = (groups * SUB * TURNED, LANES), (groups * SUB * TERMS, LANES)
    flops = rows * LANES * 40

    eps_g = 0.75 * WENO_EPS * CELL_SIZE**2
    eps_h = 0.75 * WENO_EPS * d_theta**2
    eps_v = 0.75 * WENO_EPS * d_speed**2

    ends = [
        (float(v * c / CELL_SIZE), float(v * s / CELL_SIZE))
        for v in (speeds[0], speeds[-1])
        for c, s in zip(cosines, sines)
    ]
    copies = pltpu.SemaphoreType.DMA
    wind_shape = wind_field.shape
    rate, *faces = call(
        functools.partial(
            pack_kernel, sizes=sizes, ends=ends, rest=TURN_MAX / d_theta + ACCEL_MAX / d_speed
        ),
        [start, wind_field],
        [(SUB, nv)] + face_shapes[:4],
        1000,
        hbm=2,
        scratch=[pltpu.VMEM(wind_shape, jnp.float32), copies((2 * nx + 3,))],
    )
    u, turned, wind_x, wind_y, *y_face = call(
        functools.partial(prep_kernel, sizes=sizes),
        [start, wind_field],
        [padded, turned_shape, (nx * ny, nv), (ny * nx, nv)] + face_shapes[4:],
        1000,
        hbm=2,
        scratch=[
            pltpu.VMEM(wind_shape, jnp.float32),
            pltpu.VMEM((ny * nx, nv), jnp.float32),
            copies((nx + 1,)),
        ],
    )
    faces += y_face
    rate = all_max(rate)
    first = u
    for stage in (1, 2, 3):
        got_x = neighbours(faces[0], faces[1], "gx", False)
        got_h = neighbours(faces[2], faces[3], "ha", True)
        got_y = neighbours(faces[4], faces[5] if len(faces) > 5 else None, "gy", False)
        (terms,) = call(
            functools.partial(speed_kernel, eps=eps_v, scale=ACCEL_MAX / (6.0 * d_speed)),
            [turned],
            [terms_shape],
            flops,
        )
        (acc,) = call(
            functools.partial(y_kernel, sizes=sizes, eps=eps_g), [u, *got_y, wind_y, speed_y], [padded], flops
        )
        (acc,) = call(
            functools.partial(x_first_kernel, sizes=sizes, eps=eps_g),
            [u, got_x[0], wind_x, speed_x, acc],
            [padded],
            flops,
            aliases={4: 0},
        )
        for face_a, got in zip((True, False), got_h):
            (acc,) = call(
                functools.partial(head_kernel, sizes=sizes, eps=eps_h, scale=TURN_MAX / (6.0 * d_theta), face_a=face_a),
                [u, got, acc],
                [padded],
                flops,
                aliases={2: 0},
            )
        ins = [u, got_x[1], wind_x, speed_x, acc, terms, rate]
        if stage > 1:
            ins.append(first)
        got = call(
            functools.partial(x_kernel, sizes=sizes, eps=eps_g, stage=stage),
            ins,
            [padded, turned_shape] + face_shapes if stage < 3 else [(nx, nh * ny, nv)],
            flops,
            keep=stage < 3,
            scratch=[] if stage < 3 else [pltpu.VMEM((nx, nh * ny, nv), jnp.float32), copies((nh,))],
        )
        if stage < 3:
            u, turned, faces = got[0], got[1], got[2:]
    return got[0].reshape(nx, nh, ny, nv).transpose(0, 2, 1, 3)


def solution(mesh):
    return jax.shard_map(
        body,
        mesh=mesh,
        in_specs=(P("gx", "gy", "ha", None), P(None, "gx", "gy")),
        out_specs=P("gx", "gy", "ha", None),
        check_vma=False,
    )
```

```python
import functools
import math

import jax
import jax.numpy as jnp
import numpy as np
from jax import lax
from jax.experimental import pallas as pl
from jax.experimental.pallas import tpu as pltpu
from jax.sharding import PartitionSpec as P


CELL_SIZE = 0.05
SPEED_LOW = 0.1
SPEED_SPAN = 0.4
TURN_MAX = 1.0
ACCEL_MAX = 0.05
CFL_NUMBER = 0.5
WENO_EPS = 1e-06
SUB = 8
LANES = 128


def weno_terms(us, eps):
    n = len(us) - 6
    u = {i - 3: v for i, v in enumerate(us)}
    q = {r: u[r] - u[r - 1] for r in range(-2, n + 3)}
    p = {m: q[m + 1] - q[m] for m in range(-2, n + 2)}
    t, alpha, beta, gamma, a3, g3 = {}, {}, {}, {}, {}, {}
    for r in range(-1, n + 2):
        t[r] = p[r] - p[r - 1]
        z = 1.5 * t[r]
        base = t[r] * t[r] + ((0.75 * p[r - 1]) * p[r] + eps)
        if r <= n - 1:
            s = base + p[r] * z
            alpha[r] = pl.reciprocal(s * s)
            a3[r] = (1.0 / 3.0) * alpha[r]
        if r >= 1:
            s = base - p[r - 1] * z
            gamma[r] = pl.reciprocal(s * s)
            g3[r] = (1.0 / 3.0) * gamma[r]
        if 0 <= r <= n:
            beta[r] = pl.reciprocal(0.5 * (base * base))
    f = {m: t[m] - t[m + 1] for m in range(-1, n + 1)}
    f2 = {m: f[m] + f[m] for m in range(-1, n + 1)}
    return n, q, p, alpha, beta, gamma, a3, g3, f, f2


def line_max(us, eps):
    n, q, p, alpha, beta, gamma, a3, g3, f, f2 = weno_terms(us, eps)
    q6 = {r: 6.0 * q[r] for r in range(0, n + 1)}
    outs = []
    for i in range(n):
        er = (g3[i + 2] * f2[i + 1] + alpha[i] * f[i]) * pl.reciprocal(
            g3[i + 2] + beta[i + 1] + alpha[i])
        el = (a3[i - 1] * f2[i - 1] + gamma[i + 1] * f[i]) * pl.reciprocal(
            a3[i - 1] + beta[i] + gamma[i + 1])
        p2 = p[i] + p[i]
        outs.append(jnp.minimum((p2 - q6[i + 1]) + (p[i + 1] + er), (p2 + q6[i]) + (p[i - 1] + el)))
    return outs


def line_upwind(us, eps, flows):
    n, q, p, alpha, beta, gamma, a3, g3, f, f2 = weno_terms(us, eps)
    outs = []
    for i in range(n):
        flow = flows(i)
        right = flow > 0.0
        w1 = jnp.where(right, g3[i + 2], a3[i - 1])
        w2 = jnp.where(right, beta[i + 1], beta[i])
        w3 = jnp.where(right, alpha[i], gamma[i + 1])
        f1 = jnp.where(right, f2[i + 1], f2[i - 1])
        pn = jnp.where(right, p[i + 1], p[i - 1])
        qn = jnp.where(right, q[i + 1], q[i])
        e = (w1 * f1 + w3 * f[i]) * pl.reciprocal(w1 + w2 + w3)
        x = pn + (p[i] + p[i]) + e
        outs.append(flow * qn - jnp.abs((1.0 / 6.0) * flow) * x)
    return outs


def edge_fix(low, center_low, center_high, high, flags):
    first, last = flags
    slope = center_low[0] - center_low[1]
    low = [
        jnp.where(first, center_low[0] + reach * slope, got)
        for reach, got in zip((3.0, 2.0, 1.0), low)
    ]
    slope = center_high[1] - center_high[0]
    high = [
        jnp.where(last, center_high[1] + reach * slope, got)
        for reach, got in zip((1.0, 2.0, 3.0), high)
    ]
    return low, high


def axis_flags(axis):
    count = lax.axis_size(axis)
    at = jnp.full((SUB, LANES), lax.axis_index(axis), jnp.int32)
    even = at % 2 == 0 if paired(axis) else at >= 0
    return at == 0, at == count - 1, even


def sided(even, load, a_ref, b_ref):
    from_a, from_b = load(a_ref), load(b_ref)
    low = [jnp.where(even, b, a) for a, b in zip(from_a, from_b)]
    high = [jnp.where(even, a, b) for a, b in zip(from_a, from_b)]
    return low, high


def pitch(sizes):
    _, nh, ny = sizes
    rows = nh * ny
    while rows % 8 != 4:
        rows += 1
    return rows


BLOCK = LANES // SUB
TURNED = BLOCK + 2 * SUB + 4
TERMS = BLOCK + 4


def turn(u_ref, turned_ref, h, sizes):
    nx, _, ny = sizes
    p = pitch(sizes)
    planes = nx * ny // LANES
    per = LANES // ny
    for g in range(planes):
        mat = jnp.concatenate([u_ref[pl.ds((g * per + x) * p + h * ny, ny), :] for x in range(per)], axis=0)
        mat = mat.T
        tiles = [mat[SUB * i : SUB * (i + 1)] for i in range(LANES // SUB)]
        row = lax.broadcasted_iota(jnp.int32, (SUB, LANES), 0).astype(jnp.float32)
        edge, inner = mat[0:1], mat[1:2]
        below = edge + (float(SUB) - row) * (edge - inner)
        edge, inner = mat[LANES - 1 :], mat[LANES - 2 : LANES - 1]
        above = edge + (row + 1.0) * (edge - inner)
        tiles = [below] + tiles + [above]
        base = (h * planes + g) * SUB * TURNED
        for s in range(SUB):
            for k in range(BLOCK // SUB + 2):
                turned_ref[pl.ds(base + s * TURNED + k * SUB, SUB), :] = tiles[s * (BLOCK // SUB) + k]


def speed_kernel(turned_ref, out_ref, *, eps, scale):
    groups = turned_ref.shape[0] // (SUB * TURNED)

    def group(g, carry):
        start = g * SUB * TURNED + SUB - 3
        us = [turned_ref[pl.ds(start + j, SUB, stride=TURNED), :] for j in range(BLOCK + 6)]
        for j, value in enumerate(line_max(us, eps)):
            out_ref[pl.ds(g * SUB * TERMS + j, SUB, stride=TERMS), :] = -scale * value
        return carry

    lax.fori_loop(0, groups, group, 0)


def y_kernel(u_ref, a_ref, b_ref, wind_ref, speed_ref, acc_ref, *, sizes, eps):
    nx, nh, ny = sizes
    p = pitch(sizes)
    first, last, even = axis_flags("gy")
    head = lax.axis_index("ha") * nh
    for xg in range(nx // SUB):

        def column(h, carry):
            def rows(y):
                return pl.ds(xg * SUB * p + h * ny + y, SUB, stride=p)

            center = [u_ref[rows(y), :] for y in range(ny)]

            def halo(ref, k):
                return ref[pl.ds(pl.multiple_of((k * nh + h) * nx + xg * SUB, SUB), SUB), :]

            low, high = sided(even, lambda ref: [halo(ref, k) for k in range(3)], a_ref, b_ref)
            low, high = edge_fix(low, center[:2], center[-2:], high, (first, last))
            speed = speed_ref[pl.ds(head + h, 1), :]
            flows = lambda y: speed + wind_ref[pl.ds(y * nx + xg * SUB, SUB), :]
            for y, value in enumerate(line_upwind(low + center + high, eps, flows)):
                acc_ref[rows(y), :] = value
            return carry

        lax.fori_loop(0, nh, column, 0)


def is_even(axis):
    return lax.axis_index(axis) % 2 == 0 if paired(axis) else None


def by_parity(even, up_when_even, run):
    if even is None:
        run(up_when_even)
        return
    pl.when(even)(lambda: run(up_when_even))
    pl.when(jnp.logical_not(even))(lambda: run(not up_when_even))


def end_line(center, face, up, edge=None):
    inside = list(center) if up else list(center)[::-1]
    beyond = list(face) if up else list(face)[::-1]
    if edge is not None:
        slope = inside[-1] - inside[-2]
        beyond = [jnp.where(edge, inside[-1] + reach * slope, got) for reach, got in zip((1.0, 2.0, 3.0), beyond)]
    return inside + beyond


def head_kernel(u_ref, face_ref, acc_in, acc_ref, *, sizes, eps, scale, face_a):
    nx, nh, ny = sizes
    p = pitch(sizes)
    half = nh // 2

    def run(up):
        cells = range(half, nh) if up else range(half - 1, -1, -1)

        def line(x, carry):
            for yg in range(ny // SUB):

                def face(k):
                    return pl.ds(pl.multiple_of((x * 3 + k) * ny + yg * SUB, SUB), SUB)

                def rows(h):
                    return pl.ds(x * p + h * ny + yg * SUB, SUB)

                keep = range(half - 3, nh) if up else range(half + 3)
                inside = [u_ref[rows(h), :] for h in keep]
                us = end_line(inside, [face_ref[face(k), :] for k in range(3)], up)
                for h, value in zip(cells, line_max(us, eps)):
                    acc_ref[rows(h), :] = acc_in[rows(h), :] - scale * value
            return carry

        lax.fori_loop(0, nx, line, 0)

    by_parity(is_even("ha"), face_a, run)


def edge_mask(up):
    first, last, _ = axis_flags("gx")
    return last if up else first


def x_half(center, face, edge, up, eps, flows):
    nx = len(center)
    half = nx // 2
    cells = list(range(half, nx) if up else range(half - 1, -1, -1))
    us = end_line(center[half - 3 :] if up else center[: half + 3], face, up, edge)
    turned_flows = (lambda i: flows(cells[i])) if up else (lambda i: -flows(cells[i]))
    return dict(zip(cells, line_upwind(us, eps, turned_flows)))


def x_first_kernel(u_ref, face_ref, wind_ref, speed_ref, acc_in, acc_ref, *, sizes, eps):
    nx, nh, ny = sizes
    p = pitch(sizes)
    head = lax.axis_index("ha") * nh

    def run(up):
        edge = edge_mask(up)

        def line(h, carry):
            speed = speed_ref[pl.ds(head + h, 1), :]
            for yg in range(ny // SUB):

                def rows(x):
                    return pl.ds(x * p + h * ny + yg * SUB, SUB)

                def face(k):
                    return pl.ds(pl.multiple_of((k * nh + h) * ny + yg * SUB, SUB), SUB)

                center = [u_ref[rows(x), :] for x in range(nx)]
                flows = lambda x: speed + wind_ref[pl.ds(x * ny + yg * SUB, SUB), :]
                got = x_half(center, [face_ref[face(k), :] for k in range(3)], edge, up, eps, flows)
                for x, value in got.items():
                    acc_ref[rows(x), :] = acc_in[rows(x), :] + value
            return carry

        lax.fori_loop(0, nh, line, 0)

    by_parity(is_even("gx"), True, run)


def x_kernel(*refs, sizes, eps, stage):
    nx, nh, ny = sizes
    p = pitch(sizes)
    it = iter(refs)
    u_ref, face_ref, wind_ref, speed_ref, acc_in, terms_ref, rate_ref = (next(it) for _ in range(7))
    first_ref = next(it) if stage > 1 else u_ref
    next_ref = next(it)
    turned_ref = next(it) if stage < 3 else None
    if stage == 3:
        done_ref, sems = next(it), next(it)

        def out_copy(h):
            at = pl.ds(pl.multiple_of(h * ny, SUB), ny)
            return pltpu.make_async_copy(done_ref.at[:, at, :], next_ref.at[:, at, :], sems.at[h])

    head = lax.axis_index("ha") * nh
    step = CFL_NUMBER / rate_ref[...]
    planes = nx * ny // LANES
    per = LANES // ny

    def run(up):
        edge = edge_mask(up)

        def line(h, carry):
            if stage < 3:
                turn(next_ref, turned_ref, jnp.maximum(h - 1, 0), sizes)
            terms = []
            for g in range(planes):
                base = (h * planes + g) * SUB * TERMS
                mat = jnp.concatenate([terms_ref[pl.ds(base + s * TERMS, BLOCK), :] for s in range(SUB)], axis=0)
                terms.append(mat.T)
            speed = speed_ref[pl.ds(head + h, 1), :]
            for yg in range(ny // SUB):

                def rows(x):
                    return pl.ds(x * p + h * ny + yg * SUB, SUB)

                def face(k):
                    return pl.ds(pl.multiple_of((k * nh + h) * ny + yg * SUB, SUB), SUB)

                center = [u_ref[rows(x), :] for x in range(nx)]
                flows = lambda x: speed + wind_ref[pl.ds(x * ny + yg * SUB, SUB), :]
                got = x_half(center, [face_ref[face(k), :] for k in range(3)], edge, up, eps, flows)
                for x in range(nx):
                    at = (x % per) * ny + yg * SUB
                    total = acc_in[rows(x), :] + terms[x // per][at : at + SUB]
                    if x in got:
                        total = total + got[x]
                    change = step * jnp.minimum(total, 0.0)
                    if stage == 1:
                        new = center[x] + change
                    elif stage == 2:
                        new = 0.75 * first_ref[rows(x), :] + 0.25 * (center[x] + change)
                    else:
                        start = first_ref[rows(x), :]
                        new = (2.0 / 3.0) * ((center[x] - start) + change)
                    if stage < 3:
                        next_ref[rows(x), :] = new
                    else:
                        done_ref[x, pl.ds(pl.multiple_of(h * ny + yg * SUB, SUB), SUB), :] = new
            if stage == 3:
                out_copy(h).start()
            return carry

        lax.fori_loop(0, nh, line, 0)

    by_parity(is_even("gx"), False, run)
    if stage == 3:
        for h in range(nh):
            out_copy(h).wait()
        return
    turn(next_ref, turned_ref, nh - 1, sizes)
    pack_faces(next_ref, list(it), sizes)


def pack_faces(u_ref, faces, sizes):
    nx, nh, ny = sizes
    p = pitch(sizes)
    xa, xb, ha, hb = faces[:4]
    even = axis_flags("gx")[2]
    for k in range(3):
        for i in range(nh * ny // SUB):
            low = u_ref[pl.ds(k * p + i * SUB, SUB), :]
            high = u_ref[pl.ds((nx - 3 + k) * p + i * SUB, SUB), :]
            both(xa, xb, pl.ds(k * nh * ny + i * SUB, SUB), low, high, even)
    even_h = axis_flags("ha")[2]
    for x in range(nx):
        for k in range(3 * ny // SUB):
            low = u_ref[pl.ds(x * p + k * SUB, SUB), :]
            high = u_ref[pl.ds(x * p + (nh - 3) * ny + k * SUB, SUB), :]
            both(ha, hb, pl.ds(x * 3 * ny + k * SUB, SUB), low, high, even_h)
    y_faces(u_ref, faces[4:], sizes)


def both(a_ref, b_ref, at, low, high, even):
    a_ref[at, :] = jnp.where(even, high, low)
    if b_ref is not None:
        b_ref[at, :] = jnp.where(even, low, high)


def y_faces(u_ref, faces, sizes):
    nx, nh, ny = sizes
    p = pitch(sizes)
    ya, yb = faces[0], faces[1] if len(faces) > 1 else None
    even_y = axis_flags("gy")[2]
    for xg in range(nx // SUB):
        for h in range(nh):
            for k in range(3):

                def rows(y):
                    return pl.ds(xg * SUB * p + h * ny + y, SUB, stride=p)

                at = pl.ds((k * nh + h) * nx + xg * SUB, SUB)
                both(ya, yb, at, u_ref[rows(k), :], u_ref[rows(ny - 3 + k), :], even_y)


def pack_kernel(start_ref, wind_ref, rate_ref, xa, xb, ha, hb, wind, sems, *, sizes, ends, rest):
    nx, nh, ny = sizes
    plane, count = nh * ny, iter(range(2 * nx + 3))

    def copy(source, target):
        got = pltpu.make_async_copy(source, target, sems.at[next(count)])
        got.start()
        return got

    def side(axis, high, flip):
        even = lax.axis_index(axis) % 2 == 0 if paired(axis) else True
        return pl.multiple_of(jnp.where(jnp.logical_xor(even, flip), high, 0), SUB)

    copies = []
    for face, flip in ((hb, True), (ha, False)):
        at = side("ha", (nh - 3) * ny, flip)
        for x in range(nx):
            source = start_ref.at[pl.ds(x * plane + at, 3 * ny), :]
            copies.append(copy(source, face.at[pl.ds(x * 3 * ny, 3 * ny), :]))
    for face, flip in ((xa, False), (xb, True)):
        copies.append(copy(start_ref.at[pl.ds(side("gx", (nx - 3) * plane, flip), 3 * plane), :], face))
    copy(wind_ref, wind).wait()
    top = None
    for along_x, along_y in ends:
        rate = jnp.abs(wind[0] * (1.0 / CELL_SIZE) + along_x) + jnp.abs(wind[1] * (1.0 / CELL_SIZE) + along_y)
        top = rate if top is None else jnp.maximum(top, rate)
    rate_ref[...] = jnp.full(rate_ref.shape, jnp.max(top) + rest, jnp.float32)
    for got in copies:
        got.wait()


def prep_kernel(start_ref, wind_ref, u_ref, turned_ref, wind_x, wind_y, *refs, sizes):
    nx, nh, ny = sizes
    p = pitch(sizes)
    faces, (wind, columns, sems) = refs[:-3], refs[-3:]
    copies = [
        pltpu.make_async_copy(
            start_ref.at[pl.ds(x * nh * ny, nh * ny), :], u_ref.at[pl.ds(x * p, nh * ny), :], sems.at[x]
        )
        for x in range(nx)
    ]
    copies.append(pltpu.make_async_copy(wind_ref, wind, sems.at[nx]))
    for copy in copies:
        copy.start()
    copies[-1].wait()
    for y in range(ny):
        for k, table in enumerate((columns, wind_y)):
            column = wind[k][:, y : y + 1] * (1.0 / CELL_SIZE)
            table[pl.ds(y * nx, nx), :] = jnp.broadcast_to(column, (nx, LANES))
    for x in range(nx):
        for yg in range(ny // SUB):
            wind_x[pl.ds(x * ny + yg * SUB, SUB), :] = columns[pl.ds(yg * SUB * nx + x, SUB, stride=nx), :]
    for copy in copies[:-1]:
        copy.wait()
    y_faces(u_ref, list(faces), sizes)
    for h in range(nh):
        turn(u_ref, turned_ref, h, sizes)


VMEM_LIMIT = 8 * 1024 * 1024
VM = pl.BlockSpec(memory_space=pltpu.VMEM)


def call(kernel, ins, outs, flops, keep=True, hbm=0, scratch=(), aliases=None):
    shapes = [pltpu.VMEM(s, jnp.float32) if keep else jax.ShapeDtypeStruct(s, jnp.float32) for s in outs]
    ins = [pltpu.with_memory_space_constraint(x, pltpu.HBM) for x in ins[:hbm]] + [pltpu.with_memory_space_constraint(x, pltpu.VMEM) for x in ins[hbm:]]
    return pl.pallas_call(
        kernel,
        out_shape=shapes,
        in_specs=[pl.BlockSpec(memory_space=pltpu.HBM)] * hbm + [VM] * (len(ins) - hbm),
        out_specs=[VM if keep else pl.BlockSpec(memory_space=pltpu.HBM)] * len(outs),
        scratch_shapes=list(scratch),
        input_output_aliases=aliases or {},
        compiler_params=pltpu.CompilerParams(vmem_limit_bytes=VMEM_LIMIT),
        cost_estimate=pl.CostEstimate(flops=flops, transcendentals=0, bytes_accessed=1024),
    )(*ins)


def paired(axis):
    return lax.axis_size(axis) % 2 == 0


def neighbours(face_a, face_b, axis, closed):
    count = lax.axis_size(axis)
    ends = count if closed else count - 1

    def send(face, pairs, over=axis):
        return lax.ppermute(face, over, pairs)

    if not paired(axis):
        got_b = send(face_a, [(i, (i + 1) % count) for i in range(ends)])
        got_a = send(face_b, [((i + 1) % count, i) for i in range(ends)])
        return got_a, got_b

    def swap(face, start):
        pairs = []
        for i in range(start, ends, 2):
            pairs += [(i, (i + 1) % count), ((i + 1) % count, i)]
        alone = sorted(set(range(count)) - {i for i, _ in pairs})
        side = lax.axis_size("gy")
        if not pairs or not alone or axis != "gx" or side % 2:
            return send(face, pairs) if pairs else None
        every = [(i * side + k, j * side + k) for i, j in pairs for k in range(side)]
        every += [(i * side + k, i * side + (k ^ 1)) for i in alone for k in range(side)]
        return send(face, sorted(every), (axis, "gy"))

    got_b = swap(face_b, 1) if face_b is not None else None
    got_a = swap(face_a, 0)
    return got_a, got_a if got_b is None else got_b


def all_max(value):
    rounds = []
    for axis in ("gx", "gy"):
        count = lax.axis_size(axis)
        if count & (count - 1):
            value = lax.pmax(value, axis)
        else:
            rounds += [(axis, 1 << k) for k in range(count.bit_length() - 1)]
    rounds.sort(key=lambda step: step[0] == "gy")
    for axis, reach in rounds:
        other = lax.ppermute(value, axis, [(i, i ^ reach) for i in range(lax.axis_size(axis))])
        value = jnp.maximum(value, other)
    return value


def body(level_set, wind_field):
    nx, ny, nh, nv = level_set.shape
    sizes = (nx, nh, ny)
    rows = nx * nh * ny
    n_head = nh * lax.axis_size("ha")
    d_theta = 2.0 * math.pi / n_head
    d_speed = SPEED_SPAN / nv

    angles = np.arange(n_head) * d_theta
    cosines, sines = np.cos(angles), np.sin(angles)
    speeds = SPEED_LOW + SPEED_SPAN * (np.arange(nv) + 0.5) / nv
    speed_x = jnp.asarray(cosines[:, None] * speeds / CELL_SIZE, jnp.float32)
    speed_y = jnp.asarray(sines[:, None] * speeds / CELL_SIZE, jnp.float32)

    start = level_set.transpose(0, 2, 1, 3).reshape(rows, nv)
    x_face, h_face, y_face = (3 * nh * ny, nv), (nx * 3 * ny, nv), (3 * nh * nx, nv)
    face_shapes = [x_face, x_face, h_face, h_face] + [y_face] * (1 if lax.axis_size("gy") == 2 else 2)
    padded = (nx * pitch(sizes), nv)
    groups = rows // LANES
    turned_shape, terms_shape = (groups * SUB * TURNED, LANES), (groups * SUB * TERMS, LANES)
    flops = rows * LANES * 40

    eps_g = 0.75 * WENO_EPS * CELL_SIZE**2
    eps_h = 0.75 * WENO_EPS * d_theta**2
    eps_v = 0.75 * WENO_EPS * d_speed**2

    ends = [
        (float(v * c / CELL_SIZE), float(v * s / CELL_SIZE))
        for v in (speeds[0], speeds[-1])
        for c, s in zip(cosines, sines)
    ]
    copies = pltpu.SemaphoreType.DMA
    wind_shape = wind_field.shape
    rate, *faces = call(
        functools.partial(
            pack_kernel, sizes=sizes, ends=ends, rest=TURN_MAX / d_theta + ACCEL_MAX / d_speed
        ),
        [start, wind_field],
        [(SUB, nv)] + face_shapes[:4],
        1000,
        hbm=2,
        scratch=[pltpu.VMEM(wind_shape, jnp.float32), copies((2 * nx + 3,))],
    )
    u, turned, wind_x, wind_y, *y_face = call(
        functools.partial(prep_kernel, sizes=sizes),
        [start, wind_field],
        [padded, turned_shape, (nx * ny, nv), (ny * nx, nv)] + face_shapes[4:],
        1000,
        hbm=2,
        scratch=[
            pltpu.VMEM(wind_shape, jnp.float32),
            pltpu.VMEM((ny * nx, nv), jnp.float32),
            copies((nx + 1,)),
        ],
    )
    faces += y_face
    rate = all_max(rate)
    first = u
    for stage in (1, 2, 3):
        got_x = neighbours(faces[0], faces[1], "gx", False)
        got_h = neighbours(faces[2], faces[3], "ha", True)
        got_y = neighbours(faces[4], faces[5] if len(faces) > 5 else None, "gy", False)
        (terms,) = call(
            functools.partial(speed_kernel, eps=eps_v, scale=ACCEL_MAX / (6.0 * d_speed)),
            [turned],
            [terms_shape],
            flops,
        )
        (acc,) = call(
            functools.partial(y_kernel, sizes=sizes, eps=eps_g), [u, *got_y, wind_y, speed_y], [padded], flops
        )
        (acc,) = call(
            functools.partial(x_first_kernel, sizes=sizes, eps=eps_g),
            [u, got_x[0], wind_x, speed_x, acc],
            [padded],
            flops,
            aliases={4: 0},
        )
        for face_a, got in zip((True, False), got_h):
            (acc,) = call(
                functools.partial(head_kernel, sizes=sizes, eps=eps_h, scale=TURN_MAX / (6.0 * d_theta), face_a=face_a),
                [u, got, acc],
                [padded],
                flops,
                aliases={2: 0},
            )
        ins = [u, got_x[1], wind_x, speed_x, acc, terms, rate]
        if stage > 1:
            ins.append(first)
        got = call(
            functools.partial(x_kernel, sizes=sizes, eps=eps_g, stage=stage),
            ins,
            [padded, turned_shape] + face_shapes if stage < 3 else [(nx, nh * ny, nv)],
            flops,
            keep=stage < 3,
            scratch=[] if stage < 3 else [pltpu.VMEM((nx, nh * ny, nv), jnp.float32), copies((nh,))],
        )
        if stage < 3:
            u, turned, faces = got[0], got[1], got[2:]
    return got[0].reshape(nx, nh, ny, nv).transpose(0, 2, 1, 3)


def solution(mesh):
    return jax.shard_map(
        body,
        mesh=mesh,
        in_specs=(P("gx", "gy", "ha", None), P(None, "gx", "gy")),
        out_specs=P("gx", "gy", "ha", None),
        check_vma=False,
    )
```
